256 devices in a mesh: seq: 64 (over x, z, core), head: 4 (over y).
Axes of the slice: x: 4, y: 4, z: 8, core: 2. Of those that a mesh axis runs over, the one named last changes fastest.
Arguments:
- queries: bfloat16 [16384, 64, 128], P('seq', 'head'), may hold values from -360 to 360
- head_weights: bfloat16 [16384, 64], P('seq', 'head'), may hold values from -0.75 to 0.75
- keys: bfloat16 [16384, 128], P('seq'), may hold values from -6 to 6
- targets: bfloat16 [16384, 2048], P('seq'), may hold values from 0.0099487305 to 10
- chosen: int32 [128, 16], P('seq'), may hold values from -1 to 127, as said below
- tile_block: int32 [128], replicated, may hold values from 0 to 127, as said below
Outputs:
- query_grads: bfloat16 [16384, 64, 128], P('seq', 'head')
- weight_grads: float32 [16384, 64], P('seq', 'head')
- key_grads: float32 [16384, 128], P('seq')
- loss: float32 [], replicated
The draws below stay inside these ranges and needn't reach their ends.
Inputs may be any that keep to these rules, and one draw needn't show every extreme that they name: `tile_block`: a permutation of 0 to 127; each aligned group of 4 stored positions holds the global blocks of that same group. `chosen`: slot 0 of stored tile p is tile_block[p]; live entries of a row are distinct, none exceeds tile_block[p], and they precede the -1 entries; over all tiles of one device of seq, at most 1 distinct live block is stored on any one other device.
All inputs are finite; a program needn't handle non-finite values.
Results may differ from the reference program's by a relative error of at most 0.0095.
Values may be sent and summed in bfloat16 or wider, within the bound.
A program may use at most 128 MiB of HBM per device.

```python
import math
import jax
import jax.numpy as jnp
from jax import lax

HEADS = 64
DH = 128
BLOCK = 128
SLOTS = 16
CAP = 1
TOK_DEV = 256
GROUP = 4
TOKENS = 16384
NB = 128
KEYS = 2048


def selection(key):
    tiles_dev = TOK_DEV // BLOCK
    devices_seq = NB // tiles_dev
    positions = jnp.arange(NB, dtype=jnp.int32)
    group_ids = positions // GROUP
    shuffle = jax.random.randint(jax.random.fold_in(key, 101), (NB,), 0, 4096, dtype=jnp.int32)
    order_score = group_ids * (4096 * NB) + shuffle * NB + positions
    tile_block = jnp.argsort(order_score).astype(jnp.int32)
    home_of = jnp.argsort(tile_block).astype(jnp.int32)
    pick_noise = jax.random.randint(jax.random.fold_in(key, 102), (devices_seq, devices_seq, tiles_dev), 0, 4096, dtype=jnp.int32)
    local_iota = jnp.arange(tiles_dev, dtype=jnp.int32)
    pick_score = pick_noise * tiles_dev + local_iota
    slot_rank = jnp.sum((pick_score[:, :, None, :] > pick_score[:, :, :, None]).astype(jnp.int32), axis=3)
    device_iota = jnp.arange(devices_seq, dtype=jnp.int32)
    in_pool = (slot_rank < CAP) | (device_iota[:, None, None] == device_iota[None, :, None])
    pool_mask = in_pool.reshape(devices_seq, NB)[:, home_of]
    requester = positions // tiles_dev
    candidates = pool_mask[requester] & (positions[None, :] < tile_block[:, None])
    priority_noise = jax.random.randint(jax.random.fold_in(key, 104), (NB, NB), 0, 4096, dtype=jnp.int32)
    priority = jnp.where(candidates, priority_noise * NB + positions[None, :], -1)
    top_vals, top_index = lax.top_k(priority, SLOTS - 1)
    live_slot = top_vals >= 0
    others = jnp.where(live_slot, top_index.astype(jnp.int32), -1)
    chosen = jnp.concatenate([tile_block[:, None], others], axis=1).astype(jnp.int32)
    return (tile_block, chosen)


def draw_tile_block(key, part):
    return selection(key)[0]


def draw_chosen(key, part):
    return selection(key)[1]


def draw_queries(key, part):
    base = jax.random.normal(jax.random.fold_in(key, 11), (TOKENS, HEADS, DH), jnp.float32)
    base = jnp.clip(base, -6.0, 6.0)
    return base.astype(jnp.bfloat16)


def levels(key, shape, pieces, smallest, top_value):
    gain = 1.0
    for dim, parts in pieces:
        steps = jax.random.uniform(jax.random.fold_in(jax.random.fold_in(key, 6), dim), (parts,), jnp.float32, smallest / len(pieces), top_value / len(pieces))
        gain = gain * jnp.repeat(jnp.exp(steps), shape[dim] // parts).reshape((-1,) + (1,) * (len(shape) - 1 - dim))
    return gain


def gaussian(own_key, dims, width, most, pieces=(), held_as=jnp.bfloat16):
    array = jax.random.normal(own_key, dims, jnp.float32) * width
    if len(pieces) > 0:
        array = levels(own_key, dims, pieces, -0.22, 0.18) * array
    return jnp.clip(array, min=-most, max=most).astype(held_as)


def setup_inputs(seed: int = 0) -> dict:
    splits = jax.random.split(jax.random.key(seed), 7)
    return {
        "queries": draw_queries(jax.random.fold_in(splits[6], 71), 0),
        "head_weights": gaussian(splits[1], (TOKENS, HEADS), HEADS ** -0.5, 0.75, ((0, 64), (1, 4))),
        "keys": gaussian(splits[2], (TOKENS, DH), 1.0, 6.0, ((0, 64),)),
        "targets": jnp.clip(jnp.exp(math.log(10.0) - 6.912895 * jax.random.uniform(splits[3], (TOKENS, KEYS), jnp.float32) ** levels(splits[3], (TOKENS, KEYS), ((0, 64),), -0.2, 0.2)), 0.0099487305, 10.0).astype(jnp.bfloat16),
        "chosen": draw_chosen(jax.random.fold_in(splits[6], 71), 0),
        "tile_block": draw_tile_block(jax.random.fold_in(splits[6], 71), 0),
    }


loss_scale = 4194304.0


def reference(queries, head_weights, keys, targets, chosen, tile_block):
    score_scale = DH ** -0.5
    positions = jnp.arange(NB, dtype=jnp.int32)
    home_of = jnp.sum(jnp.where(tile_block[None, :] == positions[:, None], positions[None, :], 0), axis=1).astype(jnp.int32)
    live_slot = chosen >= 0
    position = home_of[jnp.maximum(chosen, 0)]
    key_blocks = keys.reshape(NB, BLOCK, DH)
    fetched = key_blocks[position]
    offsets = jnp.arange(BLOCK, dtype=jnp.int32)
    causal = offsets[None, :] <= offsets[:, None]
    own_slot = chosen == tile_block[:, None]
    live_mask = live_slot[:, None, :, None] & ((~own_slot)[:, None, :, None] | causal[None, :, None, :])
    live_mask = live_mask.reshape(TOKENS, KEYS)
    query_tiles = queries.reshape(NB, BLOCK, HEADS, DH)
    weight_tiles = head_weights.astype(jnp.float32).reshape(NB, BLOCK, HEADS)

    def dot_values(query_tile, key_tile):
        return jnp.einsum('qhd,kd->qhk', query_tile.astype(jnp.float32), key_tile.reshape(-1, DH).astype(jnp.float32), precision=lax.Precision.HIGHEST)

    def forward(operands):
        query_tile, weight_tile, key_tile = operands
        values = dot_values(query_tile, key_tile)
        return score_scale * jnp.sum(jnp.maximum(values, 0.0) * weight_tile[:, :, None], axis=1)

    scores = lax.map(forward, (query_tiles, weight_tiles, fetched)).reshape(TOKENS, KEYS)
    row_max = jnp.max(jnp.where(live_mask, scores, -1e30), axis=1)
    exp_terms = jnp.where(live_mask, jnp.exp(jnp.where(live_mask, scores - row_max[:, None], 0.0)), 0.0)
    row_norm = jnp.sum(exp_terms, axis=1)
    softmax_vals = exp_terms / row_norm[:, None]
    target_vals = jnp.where(live_mask, targets.astype(jnp.float32), 0.0)
    target_prob = target_vals / jnp.sum(target_vals, axis=1)[:, None]
    log_soft = scores - row_max[:, None] - jnp.log(row_norm)[:, None]
    kl_sum = jnp.sum(jnp.where(live_mask, target_prob * (jnp.log(jnp.where(live_mask, target_prob, 1.0)) - log_soft), 0.0))
    pair_count = jnp.sum(live_mask.astype(jnp.float32))
    grad_scores = loss_scale * KEYS * (softmax_vals - target_prob) / pair_count
    grad_tiles = grad_scores.reshape(NB, BLOCK, KEYS)

    def backward(operands):
        query_tile, weight_tile, key_tile, grad_tile = operands
        key_rows = key_tile.reshape(-1, DH)
        values = dot_values(query_tile, key_tile)
        weight_grad = score_scale * jnp.sum(jnp.maximum(values, 0.0) * grad_tile[:, None, :], axis=2)
        dot_grads = (score_scale * weight_tile[:, :, None] * grad_tile[:, None, :] * (values > 0).astype(jnp.float32)).astype(jnp.bfloat16)
        query_grad = jnp.einsum('qhk,kd->qhd', dot_grads.astype(jnp.float32), key_rows.astype(jnp.float32), precision=lax.Precision.HIGHEST).astype(jnp.bfloat16)
        key_grad = jnp.einsum('qhk,qhd->kd', dot_grads.astype(jnp.float32), query_tile.astype(jnp.float32), precision=lax.Precision.HIGHEST)
        return query_grad, weight_grad, key_grad.reshape(SLOTS, BLOCK, DH)

    query_grads, weight_grads, key_parts = lax.map(backward, (query_tiles, weight_tiles, fetched, grad_tiles))
    key_grads = jax.ops.segment_sum(key_parts.reshape(NB * SLOTS, BLOCK, DH), position.reshape(-1), num_segments=NB)
    return (query_grads.reshape(TOKENS, HEADS, DH), weight_grads.reshape(TOKENS, HEADS), key_grads.reshape(TOKENS, DH), KEYS * kl_sum / pair_count)
```

```python
import functools
import jax
import jax.numpy as jnp
from jax import lax
from jax.experimental import pallas as pl
from jax.experimental.pallas import tpu as pltpu
from jax.sharding import Mesh
from jax.sharding import PartitionSpec as P

BLOCK = 128
SLOTS = 16
KEYS = SLOTS * BLOCK
DH = 128
NY = 4
ROWS = 64
QUARTER = BLOCK // NY
SEQ = ("x", "z", "c")
LOSS_SCALE = 4194304.0
SCORE_SCALE = DH ** (-0.5)
MESH = pl.DeviceIdType.MESH
F32 = jnp.float32
BF16 = jnp.bfloat16


def coords(nx, nz):
    return (lax.axis_index("x"), lax.axis_index("z"), lax.axis_index("c"), lax.axis_index("y"))


def chip_at(nx, nz, x, z, i, sign):
    dx, dz = i // nz, lax.rem(i, nz)
    if sign > 0:
        return lax.rem(x + dx, nx), lax.rem(z + dz, nz)
    return lax.rem(x - dx + nx, nx), lax.rem(z - dz + nz, nz)


def greet(nx, nz, x, z, c, y):
    barrier = pltpu.get_barrier_semaphore()
    for i in range(1, NY):
        pl.semaphore_signal(
            barrier, inc=1, device_id={"y": lax.rem(y + i, NY)}, device_id_type=MESH
        )
    pl.semaphore_signal(barrier, inc=1, device_id={"c": 1 - c}, device_id_type=MESH)

    def one(i, carry):
        px, pz = chip_at(nx, nz, x, z, i, 1)
        pl.semaphore_signal(barrier, inc=1, device_id={"x": px, "z": pz}, device_id_type=MESH)
        return carry

    lax.fori_loop(1, nx * nz, one, 0)
    pl.semaphore_wait(barrier, NY + nx * nz - 1)


def home_of(blocks_s, block):
    base = (block // 4) * 4
    pos = base
    for i in range(1, 4):
        pos = pos + jnp.where(blocks_s[base + i] == block, i, 0)
    return pos


def gather_kernel(
    nx, nz, q_ref, w_ref, pay_ref, chosen_s, blocks_s,
    qx, wx, kx, cnt,
    gath, sel, lsem, qs, qr, ws, wr, ps, pr, cs, cr, ks, kr,
):
    chips = nx * nz
    x, z, c, y = coords(nx, nz)
    me = x * nz + z
    greet(nx, nz, x, z, c, y)

    def y_peer(i):
        return {"y": lax.rem(y + i, NY)}

    def q_copy(i):
        return pltpu.make_async_remote_copy(
            src_ref=q_ref.at[lax.rem(y + i, NY)], dst_ref=qx.at[y],
            send_sem=qs.at[i - 1], recv_sem=qr.at[i - 1],
            device_id=y_peer(i), device_id_type=MESH,
        )

    def w_copy(i):
        return pltpu.make_async_remote_copy(
            src_ref=w_ref.at[lax.rem(y + i, NY)], dst_ref=wx.at[y],
            send_sem=ws.at[i - 1], recv_sem=wr.at[i - 1],
            device_id=y_peer(i), device_id_type=MESH,
        )

    def plane_copy(i):
        px, pz = chip_at(nx, nz, x, z, i, 1)
        return pltpu.make_async_remote_copy(
            src_ref=pay_ref, dst_ref=gath.at[c * chips + me],
            send_sem=ps.at[i], recv_sem=pr.at[i],
            device_id={"x": px, "z": pz}, device_id_type=MESH,
        )

    def core_copy(i):
        sx, sz = chip_at(nx, nz, x, z, i, -1)
        slot = c * chips + sx * nz + sz
        return pltpu.make_async_remote_copy(
            src_ref=gath.at[slot], dst_ref=gath.at[slot],
            send_sem=cs.at[i], recv_sem=cr.at[i],
            device_id={"c": 1 - c}, device_id_type=MESH,
        )

    def own_copy():
        return pltpu.make_async_remote_copy(
            src_ref=pay_ref, dst_ref=gath.at[c * chips + me],
            send_sem=cs.at[0], recv_sem=cr.at[0],
            device_id={"c": 1 - c}, device_id_type=MESH,
        )

    lax.fori_loop(1, chips, lambda i, k: (plane_copy(i).start(), k)[1], 0)
    own_copy().start()
    for i in range(1, NY):
        w_copy(i).start()
    for i in range(1, NY):
        q_copy(i).start()
    own_q = pltpu.make_async_copy(q_ref.at[y], qx.at[y], lsem)
    own_q.start()
    wx[y] = w_ref[y]
    gath[c * chips + me] = pay_ref[...]

    def relay(i, carry):
        plane_copy(i).wait_recv()
        core_copy(i).start()
        return carry

    lax.fori_loop(1, chips, relay, 0)
    lax.fori_loop(0, chips, lambda i, k: (core_copy(i).wait_recv(), k)[1], 0)

    for tile in range(2):
        for j in range(SLOTS):
            pos = home_of(blocks_s, jnp.maximum(chosen_s[tile, j], 0))
            device = pos // 2
            slot = lax.rem(device, 2) * chips + device // 2
            part = 2 * lax.rem(pos, 2)
            sel[tile, j, 0:16] = gath[slot, part]
            sel[tile, j, 16:32] = gath[slot, part + 1]

    def k_copy(i):
        peer = lax.rem(y + i, NY)
        return pltpu.make_async_remote_copy(
            src_ref=sel.at[peer // 2], dst_ref=kx.at[:, pl.ds(pl.multiple_of(y * QUARTER, QUARTER), QUARTER), :],
            send_sem=ks.at[i - 1], recv_sem=kr.at[i - 1],
            device_id={"y": peer}, device_id_type=MESH,
        )

    for i in range(1, NY):
        k_copy(i).start()
    kx[:, pl.ds(pl.multiple_of(y * QUARTER, QUARTER), QUARTER), :] = sel[y // 2]

    def add_count(i, total):
        return total + gath[i, 4].astype(F32)

    total = lax.fori_loop(0, 2 * chips, add_count, jnp.zeros((16, 128), F32))
    tiles = 4 * chips
    cnt[...] = total[0:8] * float(BLOCK * BLOCK) - float(
        tiles * (BLOCK * BLOCK - BLOCK * (BLOCK + 1) // 2)
    )

    own_q.wait()
    own_copy().wait_send()
    lax.fori_loop(1, chips, lambda i, k: (plane_copy(i).wait_send(), core_copy(i).wait_send(), k)[2], 0)
    for i in range(1, NY):
        w_copy(i).wait()
        q_copy(i).wait()
        k_copy(i).wait()


def split3(value):
    hi = value.astype(BF16)
    rest = value - hi.astype(F32)
    mid = rest.astype(BF16)
    lo = (rest - mid.astype(F32)).astype(BF16)
    return hi.astype(F32), mid.astype(F32), lo.astype(F32)


def loss_rows(value, rows):
    hi, mid, lo = split3(value)
    row = lax.broadcasted_iota(jnp.int32, (rows, 128), 0)
    out = jnp.where(row == 0, hi, jnp.where(row == 1, mid, jnp.where(row == 2, lo, 0.0)))
    return out.astype(BF16)


def compute_kernel(
    nx, nz, q_ref, wb_ref, k_ref, t_ref, cnt_ref, chosen_s, blocks_s,
    qg, wg, dks, inv,
    kt, qt, dots, sc, gs, dkt, tgt, tsem,
):
    positions = 4 * nx * nz
    y = lax.axis_index("y")
    tile = y // 2
    tcopy = pltpu.make_async_copy(t_ref.at[y], tgt, tsem)
    tcopy.start()
    for j in range(SLOTS):
        kt[:, j * BLOCK : (j + 1) * BLOCK] = k_ref[j * BLOCK : (j + 1) * BLOCK, :].T
    for g in range(NY):
        for b in range(8):
            rows = slice(b * 128, (b + 1) * 128)
            wq = (q_ref[g, rows, :].astype(F32) * wb_ref[g, rows, :]).astype(BF16)
            qt[g, :, rows] = wq.T

    def forward(cc, carry):
        cols = pl.ds(pl.multiple_of(cc * 256, 256), 256)
        keys_t = kt[:, cols]
        for tb in range(4):
            rows = slice(tb * 256, (tb + 1) * 256)
            acc = None
            for g in range(NY):
                d = jnp.dot(q_ref[g, rows, :], keys_t, preferred_element_type=F32)
                dots[g, rows, cols] = d.astype(BF16)
                wv = wb_ref[g, rows, :]
                term = jnp.maximum(d, 0.0) * jnp.concatenate([wv, wv], axis=1)
                acc = term if acc is None else acc + term
            sc[tb * 16 : (tb + 1) * 16, cols] = (
                jnp.sum(acc.reshape(16, 16, 256), axis=1) * SCORE_SCALE
            )
        return carry

    lax.fori_loop(0, KEYS // 256, forward, 0)

    def clear(i, carry):
        inv[0, i] = 2 * SLOTS
        inv[1, i] = 2 * SLOTS
        return carry

    lax.fori_loop(0, positions, clear, 0)

    def enter(i, carry):
        ti, j = i // SLOTS, lax.rem(i, SLOTS)
        block = chosen_s[ti, j]

        @pl.when(block >= 0)
        def _():
            inv[ti, home_of(blocks_s, block)] = i

        return carry

    lax.fori_loop(0, 2 * SLOTS, enter, 0)

    tcopy.wait()
    row = lax.broadcasted_iota(jnp.int32, (ROWS, BLOCK), 0) + ROWS * lax.rem(y, 2)
    col = lax.broadcasted_iota(jnp.int32, (ROWS, BLOCK), 1)

    def live(j):
        on = jnp.where(chosen_s[tile, j] >= 0, 1, 0)
        on = jnp.full((ROWS, BLOCK), on, jnp.int32)
        if j == 0:
            on = jnp.where(col <= row, on, 0)
        return on > 0

    def part(j):
        return slice(j * BLOCK, (j + 1) * BLOCK)

    top = None
    tsum = None
    for j in range(SLOTS):
        s = jnp.where(live(j), sc[:, part(j)], -1e30)
        t = jnp.where(live(j), tgt[:, part(j)].astype(F32), 0.0)
        top = s if top is None else jnp.maximum(top, s)
        tsum = t if tsum is None else tsum + t
    row_max = jnp.max(top, axis=1, keepdims=True)
    row_t = 1.0 / jnp.sum(tsum, axis=1, keepdims=True)
    esum = None
    for j in range(SLOTS):
        e = jnp.where(live(j), jnp.exp(jnp.where(live(j), sc[:, part(j)] - row_max, 0.0)), 0.0)
        gs[:, part(j)] = e
        esum = e if esum is None else esum + e
    norm = jnp.sum(esum, axis=1, keepdims=True)
    row_n = 1.0 / norm
    lse = row_max + jnp.log(norm)
    kl = None
    for j in range(SLOTS):
        on = live(j)
        prob = jnp.where(on, tgt[:, part(j)].astype(F32) * row_t, 0.0)
        term = jnp.where(
            on, prob * (jnp.log(jnp.where(on, prob, 1.0)) - sc[:, part(j)] + lse), 0.0
        )
        kl = term if kl is None else kl + term
        gs[:, part(j)] = gs[:, part(j)] * row_n - prob
    kl_row = jnp.sum(kl, axis=0, keepdims=True)
    kl_sum = jnp.broadcast_to(jnp.sum(kl_row, axis=1, keepdims=True), (1, 128))

    scale = (LOSS_SCALE * KEYS * SCORE_SCALE) / cnt_ref[0:1, :]

    for g in range(NY):
        for t in range(ROWS):
            rows = slice(t * 16, (t + 1) * 16)
            grad = jnp.broadcast_to(gs[t : t + 1, :], (16, KEYS)).astype(BF16)
            d = dots[g, rows, :]
            dots[g, rows, :] = jnp.where(d > 0, grad, jnp.zeros_like(grad))
        a = jnp.dot(dots[g], k_ref[...], preferred_element_type=F32) * scale
        qg[g] = (a * wb_ref[g]).astype(BF16)
        wg[g] = jnp.sum((a * q_ref[g].astype(F32)).reshape(ROWS, 16, DH), axis=2)
        part_t = jnp.dot(qt[g], dots[g], preferred_element_type=F32)
        if g == 0:
            dkt[...] = part_t
        else:
            dkt[...] += part_t

    for j in range(SLOTS):
        block = (dkt[:, part(j)].T * scale).astype(BF16)
        for i in range(NY):
            dks[i, j] = block[i * QUARTER : (i + 1) * QUARTER]
    lr = loss_rows(kl_sum, QUARTER)
    for i in range(NY):
        dks[i, SLOTS] = lr


def scatter_kernel(
    nx, nz, qg_ref, wg_ref, dks_ref, inv_s, cnt_ref,
    oq, ow, ok, ol,
    yrecv, table, dsend, drecv, lsend, lrecv, pay, precv, fin,
    lsem, qs, qr, ws, wr, ds_, dr, cs, cr, ls, lr, ps, pr, fs, fr,
):
    chips = nx * nz
    x, z, c, y = coords(nx, nz)
    me = x * nz + z
    greet(nx, nz, x, z, c, y)

    def y_copy(src, dst, send, recv, i):
        return pltpu.make_async_remote_copy(
            src_ref=src.at[lax.rem(y + i, NY)], dst_ref=dst.at[y],
            send_sem=send.at[i - 1], recv_sem=recv.at[i - 1],
            device_id={"y": lax.rem(y + i, NY)}, device_id_type=MESH,
        )

    def d_copy(i):
        return y_copy(dks_ref, yrecv, ds_, dr, i)

    def q_copy(i):
        return y_copy(qg_ref, oq, qs, qr, i)

    def w_copy(i):
        return y_copy(wg_ref, ow, ws, wr, i)

    for i in range(1, NY):
        d_copy(i).start()
    for i in range(1, NY):
        w_copy(i).start()
    for i in range(1, NY):
        q_copy(i).start()
    own_q = pltpu.make_async_copy(qg_ref.at[y], oq.at[y], lsem)
    own_q.start()
    ow[y] = wg_ref[y]
    yrecv[y] = dks_ref[y]
    table[2 * SLOTS] = jnp.zeros((QUARTER, DH), F32)
    for i in range(1, NY):
        d_copy(i).wait_recv()
    for tile in range(2):
        for j in range(SLOTS):
            table[tile * SLOTS + j] = yrecv[2 * tile, j].astype(F32) + yrecv[
                2 * tile + 1, j
            ].astype(F32)
    loss4 = yrecv[0, SLOTS].astype(F32)
    for i in range(1, NY):
        loss4 = loss4 + yrecv[i, SLOTS].astype(F32)
    loss_here = jnp.sum(loss4, axis=0, keepdims=True)

    def dense(core, chip, l):
        pos = (chip * 2 + core) * 2 + l
        return table[inv_s[0, pos]] + table[inv_s[1, pos]]

    def fill(chip, carry):
        for l in range(2):
            v = dense(1 - c, chip, l).astype(BF16)
            dsend[chip, l] = v
        return carry

    lax.fori_loop(0, chips, fill, 0)
    lsend[...] = jnp.broadcast_to(loss_here, (8, 128))

    def core_copy():
        return pltpu.make_async_remote_copy(
            src_ref=dsend, dst_ref=drecv, send_sem=cs, recv_sem=cr,
            device_id={"c": 1 - c}, device_id_type=MESH,
        )

    def loss_copy():
        return pltpu.make_async_remote_copy(
            src_ref=lsend, dst_ref=lrecv, send_sem=ls, recv_sem=lr,
            device_id={"c": 1 - c}, device_id_type=MESH,
        )

    loss_copy().start()
    core_copy().start()
    loss_copy().wait_recv()
    lrows = loss_rows(loss_here + lrecv[0:1, :], 16)
    core_copy().wait_recv()

    def merge(chip, carry):
        for l in range(2):
            v = dense(c, chip, l) + drecv[chip, l].astype(F32)
            v = v.astype(BF16)
            pay[chip, 2 * l] = v[0:16]
            pay[chip, 2 * l + 1] = v[16:32]
        pay[chip, 4] = lrows
        return carry

    lax.fori_loop(0, chips, merge, 0)

    def plane_copy(i):
        px, pz = chip_at(nx, nz, x, z, i, 1)
        return pltpu.make_async_remote_copy(
            src_ref=pay.at[px * nz + pz], dst_ref=precv.at[me],
            send_sem=ps.at[i], recv_sem=pr.at[i],
            device_id={"x": px, "z": pz}, device_id_type=MESH,
        )

    lax.fori_loop(1, chips, lambda i, k: (plane_copy(i).start(), k)[1], 0)
    precv[me] = pay[me]
    lax.fori_loop(1, chips, lambda i, k: (plane_copy(i).wait_recv(), k)[1], 0)

    def add(i, total):
        return tuple(total[k] + precv[i, k].astype(F32) for k in range(5))

    total = lax.fori_loop(0, chips, add, tuple(jnp.zeros((16, DH), F32) for _ in range(5)))
    loss_all = jnp.sum(total[4], axis=0, keepdims=True)
    ol[...] = jnp.broadcast_to(loss_all, (8, 128)) * float(KEYS) / cnt_ref[...]
    for l in range(2):
        fin[l, 0:16] = total[2 * l]
        fin[l, 16:32] = total[2 * l + 1]
    mine = pl.ds(pl.multiple_of(y * QUARTER, QUARTER), QUARTER)

    def f_copy(i):
        return pltpu.make_async_remote_copy(
            src_ref=fin, dst_ref=ok.at[:, mine, :],
            send_sem=fs.at[i - 1], recv_sem=fr.at[i - 1],
            device_id={"y": lax.rem(y + i, NY)}, device_id_type=MESH,
        )

    for i in range(1, NY):
        f_copy(i).start()
    ok[:, mine, :] = fin[...]
    own_q.wait()
    core_copy().wait_send()
    loss_copy().wait_send()
    lax.fori_loop(1, chips, lambda i, k: (plane_copy(i).wait_send(), k)[1], 0)
    for i in range(1, NY):
        d_copy(i).wait_send()
        w_copy(i).wait()
        q_copy(i).wait()
        f_copy(i).wait()


VM = pl.BlockSpec(memory_space=pltpu.VMEM)
SM = pl.BlockSpec(memory_space=pltpu.SMEM)
ANY = pl.BlockSpec(memory_space=pl.ANY)
DMA = pltpu.SemaphoreType.DMA


def shape(*dims_dtype):
    return jax.ShapeDtypeStruct(dims_dtype[:-1], dims_dtype[-1])


def local(nx, nz, queries, head_weights, keys, targets, chosen, tile_block):
    chips = nx * nz
    y = lax.axis_index("y")
    heads = queries.shape[1]
    q4 = queries.reshape(NY, ROWS, heads, DH)
    w4 = head_weights.reshape(NY, ROWS, heads)
    quarter = lax.dynamic_slice_in_dim(keys.reshape(2, BLOCK, DH), y * QUARTER, QUARTER, 1)
    live_here = jnp.sum((chosen >= 0).astype(F32)).astype(BF16)
    payload = jnp.concatenate(
        [quarter.reshape(4, 16, DH), jnp.broadcast_to(live_here, (1, 16, DH))], axis=0
    )
    qx, wx, kx, cnt = pl.pallas_call(
        functools.partial(gather_kernel, nx, nz),
        out_shape=[
            shape(NY, ROWS, heads, DH, BF16),
            shape(NY, ROWS, heads, BF16),
            shape(SLOTS, BLOCK, DH, BF16),
            shape(8, 128, F32),
        ],
        in_specs=[ANY, VM, VM, SM, SM],
        out_specs=[VM, VM, VM, VM],
        scratch_shapes=[
            pltpu.VMEM((2 * chips, 5, 16, DH), BF16),
            pltpu.VMEM((2, SLOTS, QUARTER, DH), BF16),
            DMA, DMA((3,)), DMA((3,)), DMA((3,)), DMA((3,)),
            DMA((chips,)), DMA((chips,)), DMA((chips,)), DMA((chips,)),
            DMA((3,)), DMA((3,)),
        ],
        compiler_params=pltpu.CompilerParams(collective_id=0, has_side_effects=True),
        name="gather",
    )(q4, w4, payload, chosen, tile_block)
    wb = jnp.broadcast_to(wx.astype(F32)[..., None], (NY, ROWS, heads, DH))
    wb = wb.reshape(NY, ROWS * heads, DH)
    qf = qx.reshape(NY, ROWS * heads, DH)
    qg, wg, dks, inv = pl.pallas_call(
        functools.partial(compute_kernel, nx, nz),
        out_shape=[
            shape(NY, ROWS * heads, DH, BF16),
            shape(NY, ROWS, heads, F32),
            shape(NY, SLOTS + 1, QUARTER, DH, BF16),
            shape(2, 4 * chips, jnp.int32),
        ],
        in_specs=[VM, VM, VM, ANY, VM, SM, SM],
        out_specs=[VM, VM, VM, SM],
        scratch_shapes=[
            pltpu.VMEM((DH, KEYS), BF16),
            pltpu.VMEM((NY, DH, ROWS * heads), BF16),
            pltpu.VMEM((NY, ROWS * heads, KEYS), BF16),
            pltpu.VMEM((ROWS, KEYS), F32),
            pltpu.VMEM((ROWS, KEYS), F32),
            pltpu.VMEM((DH, KEYS), F32),
            pltpu.VMEM((ROWS, KEYS), BF16),
            DMA,
        ],
        compiler_params=pltpu.CompilerParams(vmem_limit_bytes=60 * 1024 * 1024),
        name="compute",
    )(qf, wb, kx.reshape(KEYS, DH), targets.reshape(NY, ROWS, KEYS), cnt, chosen, tile_block)
    oq, ow, ok, ol = pl.pallas_call(
        functools.partial(scatter_kernel, nx, nz),
        out_shape=[
            shape(NY, ROWS, heads, DH, BF16),
            shape(NY, ROWS, heads, F32),
            shape(2, BLOCK, DH, F32),
            shape(8, 128, F32),
        ],
        in_specs=[ANY, VM, VM, SM, VM],
        out_specs=[VM, VM, VM, VM],
        scratch_shapes=[
            pltpu.VMEM((NY, SLOTS + 1, QUARTER, DH), BF16),
            pltpu.VMEM((2 * SLOTS + 1, QUARTER, DH), F32),
            pltpu.VMEM((chips, 2, QUARTER, DH), BF16),
            pltpu.VMEM((chips, 2, QUARTER, DH), BF16),
            pltpu.VMEM((8, 128), F32),
            pltpu.VMEM((8, 128), F32),
            pltpu.VMEM((chips, 5, 16, DH), BF16),
            pltpu.VMEM((chips, 5, 16, DH), BF16),
            pltpu.VMEM((2, QUARTER, DH), F32),
            DMA, DMA((3,)), DMA((3,)), DMA((3,)), DMA((3,)), DMA((3,)), DMA((3,)),
            DMA, DMA, DMA, DMA, DMA((chips,)), DMA((chips,)), DMA((3,)), DMA((3,)),
        ],
        compiler_params=pltpu.CompilerParams(collective_id=1, has_side_effects=True),
        name="scatter",
    )(qg.reshape(NY, ROWS, heads, DH), wg, dks, inv, cnt)
    rows = NY * ROWS
    return (
        oq.reshape(rows, heads, DH),
        ow.reshape(rows, heads),
        ok.reshape(rows, DH),
        ol[0, 0],
    )


def solution(mesh):
    nx, nz = 4, mesh.shape["seq"] // 8
    torus = Mesh(mesh.devices.reshape(nx, nz, 2, mesh.shape["head"]), ("x", "z", "c", "y"))
    in_specs = (P(SEQ, "y", None), P(SEQ, "y"), P(SEQ, None), P(SEQ, None), P(SEQ, None), P())
    out_specs = (P(SEQ, "y", None), P(SEQ, "y"), P(SEQ, None), P())
    return jax.shard_map(
        functools.partial(local, nx, nz),
        mesh=torus, in_specs=in_specs, out_specs=out_specs, check_vma=False,
    )
```

```python
import functools
import jax
import jax.numpy as jnp
from jax import lax
from jax.experimental import pallas as pl
from jax.experimental.pallas import tpu as pltpu
from jax.sharding import Mesh
from jax.sharding import PartitionSpec as P

BLOCK = 128
SLOTS = 16
KEYS = SLOTS * BLOCK
DH = 128
NY = 4
ROWS = 64
HG = 16
RG = ROWS * HG
QUARTER = BLOCK // NY
SEQ = ("x", "z", "c")
LOSS_SCALE = 4194304.0
SCORE_SCALE = DH ** (-0.5)
MESH = pl.DeviceIdType.MESH
F32 = jnp.float32
BF16 = jnp.bfloat16
DMA = pltpu.SemaphoreType.DMA


def remote(src, dst, send, recv, device):
    return pltpu.make_async_remote_copy(
        src_ref=src, dst_ref=dst, send_sem=send, recv_sem=recv,
        device_id=device, device_id_type=MESH,
    )


def loop(lo, hi, body):
    def step(i, carry):
        body(i)
        return carry

    lax.fori_loop(lo, hi, step, 0)


class RowSum:
    def __init__(self, axis, size, refs):
        self.axis, self.size = axis, size
        self.row, self.got, self.send, self.recv = refs

    def copy(self, i):
        peer = lax.rem(lax.axis_index(self.axis) + i, self.size)
        return remote(
            self.row, self.got.at[i], self.send.at[i], self.recv.at[i], {self.axis: peer}
        )

    def start(self, value):
        self.row[...] = value
        for i in range(1, self.size):
            self.copy(i).start()

    def finish(self):
        total = self.row[...]
        for i in range(1, self.size):
            self.copy(i).wait_recv()
            total = total + self.got[i]
        return total

    def drain(self):
        for i in range(1, self.size):
            self.copy(i).wait_send()


def row_sum_scratch(size):
    return [
        pltpu.VMEM((1, 128), F32), pltpu.VMEM((size, 1, 128), F32), DMA((size,)), DMA((size,)),
    ]


def kernel(
    nx, nz, q_ref, w_ref, keys_ref, t_ref, chosen_s, blocks_s,
    oq, ow, ok, ol,
    gath, sel, qx, wx, kx, wb, qt, kt, dots, sc, gs, tgt, qg, wg, wgr, inv,
    dks, yrecv, table, dsend, drecv, pay, xrecv, zsend, zrecv, fin,
    tsem, lsem, osem, qs, qr, ws, wr, zs, zr, xs, xr, cs, cr, ks, kr,
    ds_, dr, gs_, gr, vs, vr, es, er, us, ur, hs, hr, fs, fr, *sums,
):
    chips = nx * nz
    x, z, c, y = (lax.axis_index(a) for a in ("x", "z", "c", "y"))
    other = {"c": 1 - c}
    mine = pl.ds(pl.multiple_of(y * QUARTER, QUARTER), QUARTER)
    sizes = [("z", nz), ("x", nx), ("c", 2), ("y", NY), ("z", nz), ("x", nx), ("c", 2)]
    rows_of = [
        RowSum(a, n, sums[4 * i : 4 * i + 4]) for i, (a, n) in enumerate(sizes)
    ]
    count_z, count_x, count_c, loss_y, loss_z, loss_x, loss_c = rows_of

    def near(k):
        odd = lax.rem(k, 2)
        return odd * ((k + 1) // 2) + (1 - odd) * lax.rem(nz - k // 2, nz)

    def wrap(v, n):
        return lax.rem(v + n, n)

    barrier = pltpu.get_barrier_semaphore()
    for axis, size in (("z", nz), ("x", nx), ("y", NY), ("c", 2)):
        for i in range(1, size):
            peer = lax.rem(lax.axis_index(axis) + i, size)
            pl.semaphore_signal(barrier, inc=1, device_id={axis: peer}, device_id_type=MESH)
    tcopy = pltpu.make_async_copy(t_ref.at[y], tgt, tsem)
    tcopy.start()
    own_q = pltpu.make_async_copy(q_ref.at[y], qx.at[y], lsem)
    own_q.start()
    live_here = 0
    for tile in range(2):
        for j in range(SLOTS):
            live_here = live_here + jnp.where(chosen_s[tile, j] >= 0, 1, 0)
    pl.semaphore_wait(barrier, nz + nx + NY + 2 - 4)

    def slot(core, cx, cz):
        return core * chips + cx * nz + cz

    here = slot(c, x, z)

    def z_copy(dz):
        return remote(
            keys_ref.at[:, mine, :], gath.at[here], zs.at[dz], zr.at[dz],
            {"z": lax.rem(z + dz, nz)},
        )

    def x_copy(dx, dz):
        at = slot(c, x, wrap(z - dz, nz))
        i = dx * nz + dz
        return remote(gath.at[at], gath.at[at], xs.at[i], xr.at[i], {"x": lax.rem(x + dx, nx)})

    def x_own(dx):
        return remote(
            keys_ref.at[:, mine, :], gath.at[here], xs.at[dx * nz], xr.at[dx * nz],
            {"x": lax.rem(x + dx, nx)},
        )

    def c_copy(dx, dz):
        at = slot(c, wrap(x - dx, nx), wrap(z - dz, nz))
        i = dx * nz + dz
        return remote(gath.at[at], gath.at[at], cs.at[i], cr.at[i], other)

    def c_own():
        return remote(keys_ref.at[:, mine, :], gath.at[here], cs.at[0], cr.at[0], other)

    def q_copy(i):
        peer = lax.rem(y + i, NY)
        return remote(q_ref.at[peer], qx.at[y], qs.at[i], qr.at[i], {"y": peer})

    def w_copy(i):
        peer = lax.rem(y + i, NY)
        return remote(w_ref.at[peer // 2], wx.at[y], ws.at[i], wr.at[i], {"y": peer})

    loop(1, nz, lambda k: z_copy(near(nz - k)).start())
    for dx in (2, 1, 3):
        x_own(dx).start()
    c_own().start()
    for i in (2, 1, 3):
        w_copy(i).start()
    for i in (2, 1, 3):
        q_copy(i).start()
    count_z.start(jnp.full((1, 128), live_here, jnp.int32).astype(F32))
    gath[here] = keys_ref[:, mine, :]
    wx[y] = w_ref[y // 2]

    def relay_z(k):
        dz = near(k)
        z_copy(dz).wait_recv()
        for dx in (2, 1, 3):
            x_copy(dx, dz).start()
        c_copy(0, dz).start()

    loop(1, nz, relay_z)
    count_x.start(count_z.finish())

    def invert(p):
        block = blocks_s[p]
        for tile in range(2):
            at = 2 * SLOTS
            for j in range(SLOTS):
                at = jnp.where(chosen_s[tile, j] == block, tile * SLOTS + j, at)
            inv[tile, p] = at

    loop(0, 4 * chips, invert)

    def relay_x(k):
        dz = near(k)
        for dx in (1, 3, 2):
            i = dx * nz + dz
            x_copy(dx, dz).wait_recv()
            c_copy(dx, dz).start()

    loop(0, nz, relay_x)
    count_c.start(count_x.finish())
    loop(0, chips, lambda i: c_copy(i // nz, lax.rem(i, nz)).wait_recv())

    for tile in range(2):
        for j in range(SLOTS):
            block = jnp.maximum(chosen_s[tile, j], 0)
            base = (block // 4) * 4
            pos = base
            for i in range(1, 4):
                pos = pos + jnp.where(blocks_s[base + i] == block, i, 0)
            device = pos // 2
            at = lax.rem(device, 2) * chips + device // 2
            sel[tile, j] = gath[at, lax.rem(pos, 2)]

    def k_copy(i):
        peer = lax.rem(y + i, NY)
        return remote(sel.at[peer // 2], kx.at[:, mine, :], ks.at[i], kr.at[i], {"y": peer})

    for i in (2, 1, 3):
        k_copy(i).start()
    kx[:, mine, :] = sel[y // 2]

    tile = y // 2
    half = lax.rem(y, 2) * ROWS
    for i in range(1, NY):
        w_copy(i).wait_recv()
    pick = (
        lax.broadcasted_iota(jnp.int32, (RG, BLOCK), 0) // HG + half
        == lax.broadcasted_iota(jnp.int32, (RG, BLOCK), 1)
    ).astype(F32).astype(BF16)
    head_lane = lax.rem(
        lax.broadcasted_iota(jnp.int32, (RG, BLOCK), 0), HG
    ) == lax.broadcasted_iota(jnp.int32, (RG, BLOCK), 1)
    ones = jnp.ones((BLOCK, BLOCK), BF16)
    for g in range(NY):
        wt = wx[g].astype(F32)
        wt = jnp.concatenate([wt, jnp.zeros((BLOCK - HG, BLOCK), F32)], axis=0).T.astype(BF16)
        row = jnp.dot(pick, wt, preferred_element_type=F32)
        row = jnp.where(head_lane, row, 0.0).astype(BF16)
        wb[g] = jnp.dot(row, ones, preferred_element_type=F32)
    own_q.wait()
    for i in range(1, NY):
        q_copy(i).wait_recv()
    for g in range(NY):
        for b in range(8):
            rows = slice(b * 128, (b + 1) * 128)
            wq = (qx[g, 8 * b : 8 * b + 8].reshape(128, DH).astype(F32) * wb[g, rows, :]).astype(BF16)
            qt[:, g * RG + b * 128 : g * RG + (b + 1) * 128] = wq.T
    count = count_c.finish() * float(BLOCK * BLOCK) - float(
        4 * chips * (BLOCK * BLOCK - BLOCK * (BLOCK + 1) // 2)
    )
    scale = (LOSS_SCALE * KEYS * SCORE_SCALE) / count
    for i in range(1, NY):
        k_copy(i).wait_recv()
    for j in range(SLOTS):
        kt[:, j * BLOCK : (j + 1) * BLOCK] = kx[j].T

    def forward(cc):
        cols = pl.ds(pl.multiple_of(cc * 256, 256), 256)
        keys_t = kt[:, cols]
        for tb in range(4):
            rows = slice(tb * 256, (tb + 1) * 256)
            acc = None
            for g in range(NY):
                qv = qx[g, 16 * tb : 16 * tb + 16].reshape(256, DH)
                d = jnp.dot(qv, keys_t, preferred_element_type=F32)
                dots[g * RG + tb * 256 : g * RG + (tb + 1) * 256, cols] = d.astype(BF16)
                wv = wb[g, rows, :]
                term = jnp.maximum(d, 0.0) * jnp.concatenate([wv, wv], axis=1)
                acc = term if acc is None else acc + term
            sc[tb * 16 : (tb + 1) * 16, cols] = (
                jnp.sum(acc.reshape(16, 16, 256), axis=1) * SCORE_SCALE
            )

    loop(0, KEYS // 256, forward)

    tcopy.wait()
    row = lax.broadcasted_iota(jnp.int32, (ROWS, BLOCK), 0) + half
    col = lax.broadcasted_iota(jnp.int32, (ROWS, BLOCK), 1)

    def live(j):
        on = jnp.full((ROWS, BLOCK), jnp.where(chosen_s[tile, j] >= 0, 1, 0), jnp.int32)
        if j == 0:
            on = jnp.where(col <= row, on, 0)
        return on > 0

    def part(j):
        return slice(j * BLOCK, (j + 1) * BLOCK)

    top = None
    tsum = None
    for j in range(SLOTS):
        s = jnp.where(live(j), sc[:, part(j)], -1e30)
        t = jnp.where(live(j), tgt[:, part(j)].astype(F32), 0.0)
        top = s if top is None else jnp.maximum(top, s)
        tsum = t if tsum is None else tsum + t
    row_max = jnp.max(top, axis=1, keepdims=True)
    row_t = 1.0 / jnp.sum(tsum, axis=1, keepdims=True)
    esum = None
    for j in range(SLOTS):
        e = jnp.where(live(j), jnp.exp(jnp.where(live(j), sc[:, part(j)] - row_max, 0.0)), 0.0)
        gs[:, part(j)] = e
        esum = e if esum is None else esum + e
    norm = jnp.sum(esum, axis=1, keepdims=True)
    row_n = 1.0 / norm
    lse = row_max + jnp.log(norm)
    kl = None
    for j in range(SLOTS):
        on = live(j)
        prob = jnp.where(on, tgt[:, part(j)].astype(F32) * row_t, 0.0)
        term = jnp.where(
            on, prob * (jnp.log(jnp.where(on, prob, 1.0)) - sc[:, part(j)] + lse), 0.0
        )
        kl = term if kl is None else kl + term
        gs[:, part(j)] = gs[:, part(j)] * row_n - prob
    kl_row = jnp.sum(kl, axis=0, keepdims=True)
    loss_y.start(jnp.broadcast_to(jnp.sum(kl_row, axis=1, keepdims=True), (1, 128)))

    def mask(i):
        for u in range(8):
            grad = jnp.broadcast_to(gs[pl.ds(i * 8 + u, 1), :], (HG, KEYS)).astype(BF16)
            for g in range(NY):
                at = pl.ds(pl.multiple_of(g * RG + i * 128 + u * HG, HG), HG)
                d = dots[at, :]
                dots[at, :] = jnp.where(d > 0, grad, jnp.zeros_like(grad))

    loop(0, ROWS // 8, mask)
    loss_z.start(loss_y.finish())

    def d_copy(i, part_of):
        peer = lax.rem(y + i, NY)
        some = pl.ds(part_of * (SLOTS // 2), SLOTS // 2)
        at = part_of * NY + i
        return remote(
            dks.at[peer, some], yrecv.at[y, some], ds_.at[at], dr.at[at], {"y": peer}
        )

    for part_of in range(2):
        def key_grad(cc):
            cols = pl.ds(pl.multiple_of(cc * 256, 256), 256)
            got = jnp.dot(qt[...], dots[:, cols], preferred_element_type=F32)
            for u in range(2):
                block = (got[:, u * 128 : (u + 1) * 128].T * scale).astype(BF16)
                for i in range(NY):
                    dks[i, cc * 2 + u] = block[i * QUARTER : (i + 1) * QUARTER]

        loop(part_of * 4, part_of * 4 + 4, key_grad)
        for i in (2, 1, 3):
            d_copy(i, part_of).start()
    loss_x.start(loss_z.finish())

    def qg_copy(i):
        peer = lax.rem(y + i, NY)
        return remote(qg.at[peer], oq.at[y], gs_.at[i], gr.at[i], {"y": peer})

    def wg_copy(i):
        peer = lax.rem(y + i, NY)
        return remote(wg.at[peer], wgr.at[y], vs.at[i], vr.at[i], {"y": peer})

    keys2 = kx[...].reshape(KEYS, DH)
    for i in (2, 1, 3, 0):
        g = lax.rem(y + i, NY)
        rows = pl.ds(pl.multiple_of(g * RG, RG), RG)
        a = jnp.dot(dots[rows, :], keys2, preferred_element_type=F32) * scale
        qg[g] = (a * wb[g]).astype(BF16).reshape(ROWS, HG, DH)
        s = jnp.sum(a.reshape(ROWS, HG, DH) * qx[g].astype(F32), axis=2).T
        nil = jnp.zeros((HG, ROWS), F32)
        wg[g] = jnp.where(
            half == 0, jnp.concatenate([s, nil], axis=1), jnp.concatenate([nil, s], axis=1)
        )
        if i > 0:
            wg_copy(i).start()
            qg_copy(i).start()
    own_o = pltpu.make_async_copy(qg.at[y], oq.at[y], osem)
    own_o.start()
    wgr[y] = wg[y]
    loss_c.start(loss_x.finish())

    yrecv[y] = dks[y]
    table[2 * SLOTS] = jnp.zeros((QUARTER, DH), F32)
    for part_of in range(2):
        for i in range(1, NY):
            d_copy(i, part_of).wait_recv()
    for t in range(2):
        def pair(j):
            table[t * SLOTS + j] = yrecv[2 * t, j].astype(F32) + yrecv[2 * t + 1, j].astype(F32)

        loop(0, SLOTS, pair)

    def dense(core, cx, dz, l):
        pos = slot(0, cx, lax.rem(z + dz, nz)) * 4 + core * 2 + l
        return table[inv[0, pos]] + table[inv[1, pos]]

    def e_copy(dz):
        return remote(dsend.at[dz], drecv.at[dz], es.at[dz], er.at[dz], other)

    def u_copy(dx, dz):
        to = lax.rem(x + dx, nx)
        i = dx * nz + dz
        return remote(pay.at[dz, to], xrecv.at[dx, dz], us.at[i], ur.at[i], {"x": to})

    def h_copy(dz):
        return remote(
            zsend.at[dz], zrecv.at[dz], hs.at[dz], hr.at[dz], {"z": lax.rem(z + dz, nz)}
        )

    def to_core(k):
        dz = near(nz - 1 - k)
        for cx in range(nx):
            for l in range(2):
                dsend[dz, cx, l] = dense(1 - c, cx, dz, l).astype(BF16)
        e_copy(dz).start()

    loop(0, nz, to_core)

    def to_x(k):
        dz = near(nz - 1 - k)
        e_copy(dz).wait_recv()
        for cx in range(nx):
            for l in range(2):
                v = dense(c, cx, dz, l) + drecv[dz, cx, l].astype(F32)
                pay[dz, cx, l] = v.astype(BF16)
        for dx in (2, 1, 3):
            u_copy(dx, dz).start()

    loop(0, nz, to_x)
    loss = loss_c.finish() * float(KEYS) / count
    ol[...] = jnp.broadcast_to(loss, (8, 128))

    def x_total(dz):
        total = pay[dz, x].astype(F32)
        for dx in (1, 3, 2):
            u_copy(dx, dz).wait_recv()
            total = total + xrecv[dx, dz].astype(F32)
        return total

    def to_z(k):
        dz = near(nz - 1 - k)
        zsend[dz] = x_total(dz).astype(BF16)
        h_copy(dz).start()

    loop(0, nz - 1, to_z)
    fin[...] = x_total(0)
    def add_z(k):
        dz = near(k)
        h_copy(dz).wait_recv()
        fin[...] += zrecv[dz].astype(F32)

    loop(1, nz, add_z)

    def f_copy(i):
        return remote(
            fin, ok.at[:, mine, :], fs.at[i], fr.at[i], {"y": lax.rem(y + i, NY)}
        )

    for i in (2, 1, 3):
        f_copy(i).start()
    ok[:, mine, :] = fin[...]

    for i in range(1, NY):
        wg_copy(i).wait_recv()
    ow[:, 0:128] = wgr[0] + wgr[1]
    ow[:, 128:256] = wgr[2] + wgr[3]
    own_o.wait()
    loop(1, nz, lambda dz: z_copy(dz).wait_send())
    c_own().wait_send()
    loop(1, chips, lambda i: c_copy(i // nz, lax.rem(i, nz)).wait_send())
    for dx in range(1, nx):
        loop(0, nz, lambda dz: (x_copy(dx, dz).wait_send(), u_copy(dx, dz).wait_send()))
    loop(0, nz, lambda dz: e_copy(dz).wait_send())
    loop(1, nz, lambda dz: h_copy(dz).wait_send())
    for i in range(1, NY):
        q_copy(i).wait_send()
        w_copy(i).wait_send()
        k_copy(i).wait_send()
        d_copy(i, 0).wait_send()
        d_copy(i, 1).wait_send()
        wg_copy(i).wait_send()
        qg_copy(i).wait()
        f_copy(i).wait()
    for r in rows_of:
        r.drain()


def finish_kernel(q_in, w_in, k_in, l_in, q_out, w_out, k_out, l_out):
    q_out[...] = q_in[...]
    w_out[...] = w_in[...]
    k_out[...] = k_in[...]
    l_out[0, 0] = l_in[0, 0]


VM = pl.BlockSpec(memory_space=pltpu.VMEM)
SM = pl.BlockSpec(memory_space=pltpu.SMEM)
ANY = pl.BlockSpec(memory_space=pl.ANY)


def shape(*dims_dtype):
    return jax.ShapeDtypeStruct(dims_dtype[:-1], dims_dtype[-1])


def local(nx, nz, queries, head_weights, keys, targets, chosen, tile_block):
    chips = nx * nz
    rows = NY * ROWS
    q4 = queries.reshape(NY, ROWS, HG, DH)
    w2 = jnp.stack([head_weights[:BLOCK].T, head_weights[BLOCK:].T])
    v = pltpu.VMEM
    scratch = [
        v((2 * chips, 2, QUARTER, DH), BF16),
        v((2, SLOTS, QUARTER, DH), BF16),
        v((NY, ROWS, HG, DH), BF16),
        v((NY, HG, BLOCK), BF16),
        v((SLOTS, BLOCK, DH), BF16),
        v((NY, RG, DH), F32),
        v((DH, NY * RG), BF16),
        v((DH, KEYS), BF16),
        v((NY * RG, KEYS), BF16),
        v((ROWS, KEYS), F32),
        v((ROWS, KEYS), F32),
        v((ROWS, KEYS), BF16),
        v((NY, ROWS, HG, DH), BF16),
        v((NY, HG, BLOCK), F32),
        v((NY, HG, BLOCK), F32),
        pltpu.SMEM((2, 4 * chips), jnp.int32),
        v((NY, SLOTS, QUARTER, DH), BF16),
        v((NY, SLOTS, QUARTER, DH), BF16),
        v((2 * SLOTS + 1, QUARTER, DH), F32),
        v((nz, nx, 2, QUARTER, DH), BF16),
        v((nz, nx, 2, QUARTER, DH), BF16),
        v((nz, nx, 2, QUARTER, DH), BF16),
        v((nx, nz, 2, QUARTER, DH), BF16),
        v((nz, 2, QUARTER, DH), BF16),
        v((nz, 2, QUARTER, DH), BF16),
        v((2, QUARTER, DH), F32),
        DMA, DMA, DMA,
    ]
    for n in (NY, NY, nz, chips, chips, NY, 2 * NY, NY, NY, nz, chips, nz, NY):
        scratch += [DMA((n,)), DMA((n,))]
    for n in (nz, nx, 2, NY, nz, nx, 2):
        scratch += row_sum_scratch(n)
    oq, ow, ok, ol = pl.pallas_call(
        functools.partial(kernel, nx, nz),
        out_shape=[
            shape(NY, ROWS, HG, DH, BF16),
            shape(HG, rows, F32),
            shape(2, BLOCK, DH, F32),
            shape(8, 128, F32),
        ],
        in_specs=[ANY, VM, VM, ANY, SM, SM],
        out_specs=[ANY, VM, VM, VM],
        scratch_shapes=scratch,
        compiler_params=pltpu.CompilerParams(
            collective_id=0, has_side_effects=True, vmem_limit_bytes=60 * 1024 * 1024
        ),
        name="step",
    )(q4, w2, keys.reshape(2, BLOCK, DH), targets.reshape(NY, ROWS, KEYS), chosen, tile_block)
    oq, ow, ok, ol = pl.pallas_call(
        finish_kernel,
        out_shape=[
            shape(NY, ROWS, HG, DH, BF16),
            shape(HG, rows, F32),
            shape(2, BLOCK, DH, F32),
            shape(1, 1, F32),
        ],
        in_specs=[VM, VM, VM, VM],
        out_specs=[VM, VM, VM, SM],
        name="finish",
    )(oq, ow, ok, ol)
    return oq.reshape(rows, HG, DH), ow.T, ok.reshape(rows, DH), ol[0, 0]


def solution(mesh):
    nx, nz = 4, mesh.shape["seq"] // 8
    torus = Mesh(mesh.devices.reshape(nx, nz, 2, mesh.shape["head"]), ("x", "z", "c", "y"))
    in_specs = (P(SEQ, "y", None), P(SEQ, "y"), P(SEQ, None), P(SEQ, None), P(SEQ, None), P())
    out_specs = (P(SEQ, "y", None), P(SEQ, "y"), P(SEQ, None), P())
    return jax.shard_map(
        functools.partial(local, nx, nz),
        mesh=torus, in_specs=in_specs, out_specs=out_specs, check_vma=False,
    )
```

```python
import functools
import jax
import jax.numpy as jnp
from jax import lax
from jax.experimental import pallas as pl
from jax.experimental.pallas import tpu as pltpu
from jax.sharding import Mesh
from jax.sharding import PartitionSpec as P

BLOCK = 128
SLOTS = 16
KEYS = SLOTS * BLOCK
DH = 128
NY = 4
ROWS = 64
HG = 16
RG = ROWS * HG
QUARTER = BLOCK // NY
SEQ = ("x", "z", "c")
LOSS_SCALE = 4194304.0
SCORE_SCALE = DH ** (-0.5)
MESH = pl.DeviceIdType.MESH
F32 = jnp.float32
BF16 = jnp.bfloat16
DMA = pltpu.SemaphoreType.DMA


def remote(src, dst, send, recv, device):
    return pltpu.make_async_remote_copy(
        src_ref=src, dst_ref=dst, send_sem=send, recv_sem=recv,
        device_id=device, device_id_type=MESH,
    )


def loop(lo, hi, body):
    def step(i, carry):
        body(i)
        return carry

    lax.fori_loop(lo, hi, step, 0)


class RowSum:
    def __init__(self, axis, size, refs):
        self.axis, self.size = axis, size
        self.row, self.got, self.send, self.recv = refs

    def copy(self, i):
        peer = lax.rem(lax.axis_index(self.axis) + i, self.size)
        return remote(
            self.row, self.got.at[i], self.send.at[i], self.recv.at[i], {self.axis: peer}
        )

    def start(self, value):
        self.row[...] = value
        for i in range(1, self.size):
            self.copy(i).start()

    def finish(self):
        total = self.row[...]
        for i in range(1, self.size):
            self.copy(i).wait_recv()
            total = total + self.got[i]
        return total

    def drain(self):
        for i in range(1, self.size):
            self.copy(i).wait_send()


def row_sum_scratch(size):
    return [
        pltpu.VMEM((1, 128), F32), pltpu.VMEM((size, 1, 128), F32), DMA((size,)), DMA((size,)),
    ]


def kernel(
    nx, nz, q_ref, w_ref, keys_ref, t_ref, chosen_s, blocks_s,
    oq, ow, ok, ol,
    gath, sel, qx, wx, kx, wb, qt, dots, sc, gs, traw, tgt, qg, wg, wgr, inv,
    dks, yrecv, table, dsend, drecv, pay, xrecv, zsend, zrecv, fin,
    tsem, lsem, osem, qs, qr, ws, wr, zs, zr, xs, xr, cs, cr, ks, kr,
    ds_, dr, gs_, gr, vs, vr, es, er, us, ur, hs, hr, fs, fr, *sums,
):
    chips = nx * nz
    x, z, c, y = (lax.axis_index(a) for a in ("x", "z", "c", "y"))
    other = {"c": 1 - c}
    mine = pl.ds(pl.multiple_of(y * QUARTER, QUARTER), QUARTER)
    sizes = [("z", nz), ("x", nx), ("c", 2), ("y", NY), ("z", nz), ("x", nx), ("c", 2)]
    rows_of = [
        RowSum(a, n, sums[4 * i : 4 * i + 4]) for i, (a, n) in enumerate(sizes)
    ]
    count_z, count_x, count_c, loss_y, loss_z, loss_x, loss_c = rows_of

    def near(k):
        odd = lax.rem(k, 2)
        return odd * ((k + 1) // 2) + (1 - odd) * lax.rem(nz - k // 2, nz)

    def near4(k):
        odd = lax.rem(k, 2)
        return odd * ((k + 1) // 2) + (1 - odd) * lax.rem(NY - k // 2, NY)

    def wrap(v, n):
        return lax.rem(v + n, n)

    barrier = pltpu.get_barrier_semaphore()
    for axis, size in (("z", nz), ("x", nx), ("y", NY), ("c", 2)):
        for i in range(1, size):
            peer = lax.rem(lax.axis_index(axis) + i, size)
            pl.semaphore_signal(barrier, inc=1, device_id={axis: peer}, device_id_type=MESH)
    tcopy = pltpu.make_async_copy(t_ref.at[y], traw, tsem)
    tcopy.start()
    own_q = pltpu.make_async_copy(q_ref.at[y], qx.at[y], lsem)
    own_q.start()
    live_here = 0
    for tile in range(2):
        for j in range(SLOTS):
            live_here = live_here + jnp.where(chosen_s[tile, j] >= 0, 1, 0)
    def invert(p):
        block = blocks_s[p]
        for t in range(2):
            at = 2 * SLOTS
            for j in range(SLOTS):
                at = jnp.where(chosen_s[t, j] == block, t * SLOTS + j, at)
            inv[t, p] = at

    loop(0, 2 * chips, invert)

    tcopy.wait()
    at_row = lax.broadcasted_iota(jnp.int32, (4 * BLOCK, BLOCK), 0)
    at_col = lax.broadcasted_iota(jnp.int32, (4 * BLOCK, BLOCK), 1)
    for q in range(NY):
        source = (at_col // QUARTER) * BLOCK + q * QUARTER + lax.rem(at_col, QUARTER)
        move = (at_row == source).astype(F32).astype(BF16)
        for m in range(4):
            got = jnp.dot(
                traw[:, m * 512 : (m + 1) * 512], move, preferred_element_type=F32
            )
            tgt[:, q * 512 + m * 128 : q * 512 + (m + 1) * 128] = got.astype(BF16)
    pl.semaphore_wait(barrier, nz + nx + NY + 2 - 4)

    def slot(core, cx, cz):
        return core * chips + cx * nz + cz

    here = slot(c, x, z)

    def z_copy(dz):
        return remote(
            keys_ref.at[:, mine, :], gath.at[here], zs.at[dz], zr.at[dz],
            {"z": lax.rem(z + dz, nz)},
        )

    def x_copy(dx, dz):
        at = slot(c, x, wrap(z - dz, nz))
        i = dx * nz + dz
        return remote(gath.at[at], gath.at[at], xs.at[i], xr.at[i], {"x": lax.rem(x + dx, nx)})

    def x_own(dx):
        return remote(
            keys_ref.at[:, mine, :], gath.at[here], xs.at[dx * nz], xr.at[dx * nz],
            {"x": lax.rem(x + dx, nx)},
        )

    def c_copy(dx, dz):
        at = slot(c, wrap(x - dx, nx), wrap(z - dz, nz))
        i = dx * nz + dz
        return remote(gath.at[at], gath.at[at], cs.at[i], cr.at[i], other)

    def c_own():
        return remote(keys_ref.at[:, mine, :], gath.at[here], cs.at[0], cr.at[0], other)

    def q_copy(i):
        peer = lax.rem(y + i, NY)
        return remote(q_ref.at[peer], qx.at[y], qs.at[i], qr.at[i], {"y": peer})

    def w_copy(i):
        peer = lax.rem(y + i, NY)
        lanes = pl.ds(pl.multiple_of((peer // 2) * BLOCK, BLOCK), BLOCK)
        return remote(w_ref.at[:, lanes], wx.at[y], ws.at[i], wr.at[i], {"y": peer})

    loop(1, nz, lambda k: z_copy(near(nz - k)).start())
    for dx in (2, 1, 3):
        x_own(dx).start()
    c_own().start()
    for i in (2, 1, 3):
        w_copy(i).start()
    for i in (2, 1, 3):
        q_copy(i).start()
    count_z.start(jnp.full((1, 128), live_here, jnp.int32).astype(F32))
    gath[here] = keys_ref[:, mine, :]
    wx[y] = w_ref[:, pl.ds(pl.multiple_of((y // 2) * BLOCK, BLOCK), BLOCK)]
    loop(2 * chips, 4 * chips, invert)

    def relay_z(k):
        dz = near(k)
        z_copy(dz).wait_recv()
        for dx in (2, 1, 3):
            x_copy(dx, dz).start()
        c_copy(0, dz).start()

    loop(1, nz, relay_z)
    count_x.start(count_z.finish())

    tile = y // 2
    half = lax.rem(y, 2) * ROWS
    for i in range(1, NY):
        w_copy(i).wait_recv()
    pick = (
        lax.broadcasted_iota(jnp.int32, (RG, BLOCK), 0) // HG + half
        == lax.broadcasted_iota(jnp.int32, (RG, BLOCK), 1)
    ).astype(F32).astype(BF16)
    head_lane = lax.rem(
        lax.broadcasted_iota(jnp.int32, (RG, BLOCK), 0), HG
    ) == lax.broadcasted_iota(jnp.int32, (RG, BLOCK), 1)
    ones = jnp.ones((BLOCK, BLOCK), BF16)
    for g in range(NY):
        wt = wx[g].astype(F32)
        wt = jnp.concatenate([wt, jnp.zeros((BLOCK - HG, BLOCK), F32)], axis=0).T.astype(BF16)
        row = jnp.dot(pick, wt, preferred_element_type=F32)
        row = jnp.where(head_lane, row, 0.0).astype(BF16)
        wb[g] = jnp.dot(row, ones, preferred_element_type=F32)

    def relay_x(k):
        dz = near(k)
        for dx in (1, 3, 2):
            i = dx * nz + dz
            x_copy(dx, dz).wait_recv()
            c_copy(dx, dz).start()

    loop(0, nz, relay_x)
    count_c.start(count_x.finish())
    loop(0, chips, lambda i: c_copy(i // nz, lax.rem(i, nz)).wait_recv())

    for t in range(2):
        for j in range(SLOTS):
            block = jnp.maximum(chosen_s[t, j], 0)
            base = (block // 4) * 4
            pos = base
            for i in range(1, 4):
                pos = pos + jnp.where(blocks_s[base + i] == block, i, 0)
            device = pos // 2
            at = lax.rem(device, 2) * chips + device // 2
            sel[t, j] = gath[at, lax.rem(pos, 2)]

    def k_copy(i):
        peer = lax.rem(y + i, NY)
        return remote(sel.at[peer // 2], kx.at[y], ks.at[i], kr.at[i], {"y": peer})

    for i in (2, 1, 3):
        k_copy(i).start()
    kx[y] = sel[tile]


    own_q.wait()
    for i in range(1, NY):
        q_copy(i).wait_recv()
    for g in range(NY):
        for b in range(8):
            rows = slice(b * 128, (b + 1) * 128)
            wq = (qx[g, 8 * b : 8 * b + 8].reshape(128, DH).astype(F32) * wb[g, rows, :]).astype(BF16)
            qt[:, g * RG + b * 128 : g * RG + (b + 1) * 128] = wq.T
    count = count_c.finish() * float(BLOCK * BLOCK) - float(
        4 * chips * (BLOCK * BLOCK - BLOCK * (BLOCK + 1) // 2)
    )
    scale = (LOSS_SCALE * KEYS * SCORE_SCALE) / count

    def forward(k, part_of):
        at = wrap(y - near4(k), NY)
        cols = pl.ds(pl.multiple_of(at * 512 + part_of * 256, 256), 256)
        some = pl.ds(part_of * (SLOTS // 2), SLOTS // 2)
        kv = kx[at, some].reshape(256, DH)
        keys_t = jnp.concatenate([kv[:128].T, kv[128:].T], axis=1)
        for tb in range(4):
            rows = slice(tb * 256, (tb + 1) * 256)
            acc = None
            for g in range(NY):
                qv = qx[g, 16 * tb : 16 * tb + 16].reshape(256, DH)
                d = jnp.dot(qv, keys_t, preferred_element_type=F32)
                dots[g * RG + tb * 256 : g * RG + (tb + 1) * 256, cols] = d.astype(BF16)
                wv = wb[g, rows, :]
                term = jnp.maximum(d, 0.0) * jnp.concatenate([wv, wv], axis=1)
                acc = term if acc is None else acc + term
            sc[tb * 16 : (tb + 1) * 16, cols] = (
                jnp.sum(acc.reshape(16, 16, 256), axis=1) * SCORE_SCALE
            )

    def quarter(k):
        @pl.when(k > 0)
        def _():
            k_copy(near4(k)).wait_recv()

        loop(0, 2, lambda part_of: forward(k, part_of))

    loop(0, NY, quarter)

    row = lax.broadcasted_iota(jnp.int32, (ROWS, BLOCK), 0) + half
    col = lax.broadcasted_iota(jnp.int32, (ROWS, BLOCK), 1)
    group = col // QUARTER
    chosen_on = []
    for m in range(4):
        on = jnp.zeros((ROWS, BLOCK), jnp.int32)
        for u in range(4):
            one = jnp.where(chosen_s[tile, 4 * m + u] >= 0, 1, 0)
            on = jnp.where(group == u, jnp.full((ROWS, BLOCK), one, jnp.int32), on)
        chosen_on.append(on)

    def live(p):
        q, m = p // 4, p % 4
        on = chosen_on[m]
        if m == 0:
            on = jnp.where((group > 0) | (q * QUARTER + col <= row), on, 0)
        return on > 0

    def part(j):
        return slice(j * BLOCK, (j + 1) * BLOCK)

    top = None
    tsum = None
    for j in range(SLOTS):
        s = jnp.where(live(j), sc[:, part(j)], -1e30)
        t = jnp.where(live(j), tgt[:, part(j)].astype(F32), 0.0)
        top = s if top is None else jnp.maximum(top, s)
        tsum = t if tsum is None else tsum + t
    row_max = jnp.max(top, axis=1, keepdims=True)
    row_t = 1.0 / jnp.sum(tsum, axis=1, keepdims=True)
    esum = None
    for j in range(SLOTS):
        e = jnp.where(live(j), jnp.exp(jnp.where(live(j), sc[:, part(j)] - row_max, 0.0)), 0.0)
        gs[:, part(j)] = e
        esum = e if esum is None else esum + e
    norm = jnp.sum(esum, axis=1, keepdims=True)
    row_n = 1.0 / norm
    lse = row_max + jnp.log(norm)
    kl = None
    for j in range(SLOTS):
        on = live(j)
        prob = jnp.where(on, tgt[:, part(j)].astype(F32) * row_t, 0.0)
        term = jnp.where(
            on, prob * (jnp.log(jnp.where(on, prob, 1.0)) - sc[:, part(j)] + lse), 0.0
        )
        kl = term if kl is None else kl + term
        gs[:, part(j)] = gs[:, part(j)] * row_n - prob
    kl_row = jnp.sum(kl, axis=0, keepdims=True)
    loss_y.start(jnp.broadcast_to(jnp.sum(kl_row, axis=1, keepdims=True), (1, 128)))

    def d_copy(i):
        peer = lax.rem(y + i, NY)
        return remote(dks.at[peer], yrecv.at[y], ds_.at[i], dr.at[i], {"y": peer})

    def key_grad(k, part_of):
        at = lax.rem(y + near4(NY - 1 - k), NY)
        cols = pl.ds(pl.multiple_of(at * 512 + part_of * 256, 256), 256)
        got = None
        for tb in range(4):
            grad = jnp.concatenate(
                [
                    jnp.broadcast_to(gs[tb * 16 + u : tb * 16 + u + 1, cols], (HG, 256)).astype(BF16)
                    for u in range(16)
                ],
                axis=0,
            )
            for g in range(NY):
                rows = slice(g * RG + tb * 256, g * RG + (tb + 1) * 256)
                d = dots[rows, cols]
                d = jnp.where(d > 0, grad, jnp.zeros_like(grad))
                dots[rows, cols] = d
                term = jnp.dot(qt[:, rows], d, preferred_element_type=F32)
                got = term if got is None else got + term
        for u in range(2):
            block = (got[:, u * 128 : (u + 1) * 128].T * scale).astype(BF16)
            dks[at, pl.ds(part_of * 8 + u * 4, 4)] = block.reshape(4, QUARTER, DH)

    def key_quarter(k):
        loop(0, 2, lambda part_of: key_grad(k, part_of))

        @pl.when(k < NY - 1)
        def _():
            d_copy(near4(NY - 1 - k)).start()

    loop(0, NY, key_quarter)
    loss_z.start(loss_y.finish())

    def qg_copy(i):
        peer = lax.rem(y + i, NY)
        return remote(qg.at[peer], oq.at[y], gs_.at[i], gr.at[i], {"y": peer})

    def wg_copy(i):
        peer = lax.rem(y + i, NY)
        return remote(wg.at[peer], wgr.at[y], vs.at[i], vr.at[i], {"y": peer})

    def query_grad(i):
        g = lax.rem(y + i, NY)
        rows = pl.ds(pl.multiple_of(g * RG, RG), RG)
        a = jnp.dot(dots[rows, :], kx[...].reshape(KEYS, DH), preferred_element_type=F32) * scale
        qg[g] = (a * wb[g]).astype(BF16).reshape(ROWS, HG, DH)
        s = jnp.sum(a.reshape(ROWS, HG, DH) * qx[g].astype(F32), axis=2).T
        nil = jnp.zeros((HG, ROWS), F32)
        wg[g] = jnp.where(
            half == 0, jnp.concatenate([s, nil], axis=1), jnp.concatenate([nil, s], axis=1)
        )

    for i in (2, 1, 3):
        query_grad(i)
        wg_copy(i).start()
        qg_copy(i).start()
    loss_x.start(loss_z.finish())
    loop(1, nz, lambda dz: z_copy(dz).wait_send())
    c_own().wait_send()
    loop(1, chips, lambda i: c_copy(i // nz, lax.rem(i, nz)).wait_send())
    loop(nz, chips, lambda i: x_copy(i // nz, lax.rem(i, nz)).wait_send())
    for i in range(1, NY):
        q_copy(i).wait_send()
        w_copy(i).wait_send()
        k_copy(i).wait_send()
    for r in rows_of[:3]:
        r.drain()

    yrecv[y] = dks[y]
    table[2 * SLOTS] = jnp.zeros((QUARTER, DH), F32)
    for i in range(1, NY):
        d_copy(i).wait_recv()
    for t in range(2):
        def pair(j):
            table[t * SLOTS + j] = yrecv[2 * t, j].astype(F32) + yrecv[2 * t + 1, j].astype(F32)

        loop(0, SLOTS, pair)

    def dense(core, cx, dz, l):
        pos = slot(0, cx, lax.rem(z + dz, nz)) * 4 + core * 2 + l
        return table[inv[0, pos]] + table[inv[1, pos]]

    def e_copy(dz):
        return remote(dsend.at[dz], drecv.at[dz], es.at[dz], er.at[dz], other)

    def u_copy(dx, dz):
        to = lax.rem(x + dx, nx)
        i = dx * nz + dz
        return remote(pay.at[dz, to], xrecv.at[dx, dz], us.at[i], ur.at[i], {"x": to})

    def h_copy(dz):
        return remote(
            zsend.at[dz], zrecv.at[dz], hs.at[dz], hr.at[dz], {"z": lax.rem(z + dz, nz)}
        )

    def to_core(k):
        dz = near(nz - 1 - k)
        for cx in range(nx):
            for l in range(2):
                dsend[dz, cx, l] = dense(1 - c, cx, dz, l).astype(BF16)
        e_copy(dz).start()

    loop(0, nz, to_core)
    query_grad(0)
    own_o = pltpu.make_async_copy(qg.at[y], oq.at[y], osem)
    own_o.start()
    wgr[y] = wg[y]
    loss_c.start(loss_x.finish())

    def to_x(k):
        dz = near(nz - 1 - k)
        e_copy(dz).wait_recv()
        for cx in range(nx):
            for l in range(2):
                v = dense(c, cx, dz, l) + drecv[dz, cx, l].astype(F32)
                pay[dz, cx, l] = v.astype(BF16)
        for dx in (2, 1, 3):
            u_copy(dx, dz).start()

    loop(0, nz, to_x)
    loss = loss_c.finish() * float(KEYS) / count
    ol[...] = jnp.broadcast_to(loss, (8, 128))

    def x_total(dz):
        total = pay[dz, x].astype(F32)
        for dx in (1, 3, 2):
            u_copy(dx, dz).wait_recv()
            total = total + xrecv[dx, dz].astype(F32)
        return total

    def to_z(k):
        dz = near(nz - 1 - k)
        zsend[dz] = x_total(dz).astype(BF16)
        h_copy(dz).start()

    loop(0, nz - 1, to_z)
    fin[...] = x_total(0)
    def add_z(k):
        dz = near(k)
        h_copy(dz).wait_recv()
        fin[...] += zrecv[dz].astype(F32)

    loop(1, nz, add_z)

    def f_copy(i):
        return remote(
            fin, ok.at[:, mine, :], fs.at[i], fr.at[i], {"y": lax.rem(y + i, NY)}
        )

    for i in (2, 1, 3):
        f_copy(i).start()
    ok[:, mine, :] = fin[...]

    for i in range(1, NY):
        wg_copy(i).wait_recv()
    ow[:, 0:128] = wgr[0] + wgr[1]
    ow[:, 128:256] = wgr[2] + wgr[3]
    own_o.wait()
    loop(nz, chips, lambda i: u_copy(i // nz, lax.rem(i, nz)).wait_send())
    loop(0, nz, lambda dz: e_copy(dz).wait_send())
    loop(1, nz, lambda dz: h_copy(dz).wait_send())
    for r in rows_of[3:]:
        r.drain()
    for i in range(1, NY):
        d_copy(i).wait_send()
        wg_copy(i).wait_send()
        qg_copy(i).wait()
    for i in range(1, NY):
        f_copy(i).wait()


def finish_kernel(q_in, w_in, k_in, l_in, q_out, w_out, k_out, l_out, hold, isem, osem):
    def take(g):
        return pltpu.make_async_copy(q_in.at[g], hold.at[g], isem.at[g])

    def put(g):
        return pltpu.make_async_copy(hold.at[g], q_out.at[g], osem.at[g])

    for g in range(NY):
        take(g).start()
    w_out[...] = w_in[...]
    k_out[...] = k_in[...]
    l_out[0, 0] = l_in[0, 0]
    for g in range(NY):
        take(g).wait()
        put(g).start()
    for g in range(NY):
        put(g).wait()


VM = pl.BlockSpec(memory_space=pltpu.VMEM)
SM = pl.BlockSpec(memory_space=pltpu.SMEM)
ANY = pl.BlockSpec(memory_space=pl.ANY)


def shape(*dims_dtype):
    return jax.ShapeDtypeStruct(dims_dtype[:-1], dims_dtype[-1])


def local(nx, nz, queries, head_weights, keys, targets, chosen, tile_block):
    chips = nx * nz
    rows = NY * ROWS
    q4 = queries.reshape(NY, ROWS, HG, DH)
    v = pltpu.VMEM
    scratch = [
        v((2 * chips, 2, QUARTER, DH), BF16),
        v((2, SLOTS, QUARTER, DH), BF16),
        v((NY, ROWS, HG, DH), BF16),
        v((NY, HG, BLOCK), BF16),
        v((NY, SLOTS, QUARTER, DH), BF16),
        v((NY, RG, DH), F32),
        v((DH, NY * RG), BF16),
        v((NY * RG, KEYS), BF16),
        v((ROWS, KEYS), F32),
        v((ROWS, KEYS), F32),
        v((ROWS, KEYS), BF16),
        v((ROWS, KEYS), BF16),
        v((NY, ROWS, HG, DH), BF16),
        v((NY, HG, BLOCK), F32),
        v((NY, HG, BLOCK), F32),
        pltpu.SMEM((2, 4 * chips), jnp.int32),
        v((NY, SLOTS, QUARTER, DH), BF16),
        v((NY, SLOTS, QUARTER, DH), BF16),
        v((2 * SLOTS + 1, QUARTER, DH), F32),
        v((nz, nx, 2, QUARTER, DH), BF16),
        v((nz, nx, 2, QUARTER, DH), BF16),
        v((nz, nx, 2, QUARTER, DH), BF16),
        v((nx, nz, 2, QUARTER, DH), BF16),
        v((nz, 2, QUARTER, DH), BF16),
        v((nz, 2, QUARTER, DH), BF16),
        v((2, QUARTER, DH), F32),
        DMA, DMA, DMA,
    ]
    for n in (NY, NY, nz, chips, chips, NY, NY, NY, NY, nz, chips, nz, NY):
        scratch += [DMA((n,)), DMA((n,))]
    for n in (nz, nx, 2, NY, nz, nx, 2):
        scratch += row_sum_scratch(n)
    oq, ow, ok, ol = pl.pallas_call(
        functools.partial(kernel, nx, nz),
        out_shape=[
            shape(NY, ROWS, HG, DH, BF16),
            shape(HG, rows, F32),
            shape(2, BLOCK, DH, F32),
            shape(8, 128, F32),
        ],
        in_specs=[ANY, VM, VM, ANY, SM, SM],
        out_specs=[ANY, VM, VM, VM],
        scratch_shapes=scratch,
        compiler_params=pltpu.CompilerParams(
            collective_id=0, has_side_effects=True, vmem_limit_bytes=60 * 1024 * 1024
        ),
        name="step",
    )(q4, head_weights.T, keys.reshape(2, BLOCK, DH), targets.reshape(NY, ROWS, KEYS), chosen, tile_block)
    oq, ow, ok, ol = pl.pallas_call(
        finish_kernel,
        out_shape=[
            shape(NY, ROWS, HG, DH, BF16),
            shape(HG, rows, F32),
            shape(2, BLOCK, DH, F32),
            shape(1, 1, F32),
        ],
        in_specs=[ANY, VM, VM, VM],
        out_specs=[ANY, VM, VM, SM],
        scratch_shapes=[v((NY, ROWS, HG, DH), BF16), DMA((NY,)), DMA((NY,))],
        name="finish",
    )(oq, ow, ok, ol)
    return oq.reshape(rows, HG, DH), ow.T, ok.reshape(rows, DH), ol[0, 0]


def solution(mesh):
    nx, nz = 4, mesh.shape["seq"] // 8
    torus = Mesh(mesh.devices.reshape(nx, nz, 2, mesh.shape["head"]), ("x", "z", "c", "y"))
    in_specs = (P(SEQ, "y", None), P(SEQ, "y"), P(SEQ, None), P(SEQ, None), P(SEQ, None), P())
    out_specs = (P(SEQ, "y", None), P(SEQ, "y"), P(SEQ, None), P())
    return jax.shard_map(
        functools.partial(local, nx, nz),
        mesh=torus, in_specs=in_specs, out_specs=out_specs, check_vma=False,
    )
```

```python
import functools
import jax
import jax.numpy as jnp
from jax import lax
from jax.experimental import pallas as pl
from jax.experimental.pallas import tpu as pltpu
from jax.sharding import Mesh
from jax.sharding import PartitionSpec as P

BLOCK = 128
SLOTS = 16
KEYS = SLOTS * BLOCK
DH = 128
NY = 4
ROWS = 64
HG = 16
RG = ROWS * HG
QUARTER = BLOCK // NY
SEQ = ("x", "z", "c")
LOSS_SCALE = 4194304.0
SCORE_SCALE = DH ** (-0.5)
MESH = pl.DeviceIdType.MESH
F32 = jnp.float32
BF16 = jnp.bfloat16
DMA = pltpu.SemaphoreType.DMA


def remote(src, dst, send, recv, device):
    return pltpu.make_async_remote_copy(
        src_ref=src, dst_ref=dst, send_sem=send, recv_sem=recv,
        device_id=device, device_id_type=MESH,
    )


def loop(lo, hi, body):
    def step(i, carry):
        body(i)
        return carry

    lax.fori_loop(lo, hi, step, 0)


class RowSum:
    def __init__(self, axis, size, refs):
        self.axis, self.size = axis, size
        self.row, self.got, self.send, self.recv = refs

    def copy(self, i):
        peer = lax.rem(lax.axis_index(self.axis) + i, self.size)
        return remote(
            self.row, self.got.at[i], self.send.at[i], self.recv.at[i], {self.axis: peer}
        )

    def start(self, value):
        self.row[...] = value
        for i in range(1, self.size):
            self.copy(i).start()

    def finish(self):
        total = self.row[...]
        for i in range(1, self.size):
            self.copy(i).wait_recv()
            total = total + self.got[i]
        return total

    def drain(self):
        for i in range(1, self.size):
            self.copy(i).wait_send()


def row_sum_scratch(size):
    return [
        pltpu.VMEM((1, 128), F32), pltpu.VMEM((size, 1, 128), F32), DMA((size,)), DMA((size,)),
    ]


def kernel(
    nx, nz, q_ref, w_hbm, keys_hbm, t_ref, chosen_s, blocks_s,
    oq, ow, ok, ol,
    w_ref, keys_ref, ow_v, ol_v, fin_b, isem, rsem, gath, sel, qx, wx, kx, wb, qt, dots, sc, gs, traw, tgt, qg, wg, wgr, inv,
    dks, yrecv, table, dsend, drecv, pay, xrecv, zsend, zrecv, fin,
    tsem, lsem, osem, qs, qr, ws, wr, zs, zr, xs, xr, cs, cr, ks, kr,
    ds_, dr, gs_, gr, vs, vr, es, er, us, ur, hs, hr, fs, fr, *sums,
):
    chips = nx * nz
    x, z, c, y = (lax.axis_index(a) for a in ("x", "z", "c", "y"))
    other = {"c": 1 - c}
    tile = y // 2
    half = lax.rem(y, 2) * ROWS
    mine = pl.ds(pl.multiple_of(y * QUARTER, QUARTER), QUARTER)
    sizes = [("z", nz), ("x", nx), ("c", 2), ("y", NY), ("z", nz), ("x", nx), ("c", 2)]
    rows_of = [
        RowSum(a, n, sums[4 * i : 4 * i + 4]) for i, (a, n) in enumerate(sizes)
    ]
    count_z, count_x, count_c, loss_y, loss_z, loss_x, loss_c = rows_of

    def near(k):
        odd = lax.rem(k, 2)
        return odd * ((k + 1) // 2) + (1 - odd) * lax.rem(nz - k // 2, nz)

    def near4(k):
        odd = lax.rem(k, 2)
        return odd * ((k + 1) // 2) + (1 - odd) * lax.rem(NY - k // 2, NY)

    def wrap(v, n):
        return lax.rem(v + n, n)

    barrier = pltpu.get_barrier_semaphore()
    for axis, size in (("z", nz), ("x", nx), ("y", NY), ("c", 2)):
        for i in range(1, size):
            peer = lax.rem(lax.axis_index(axis) + i, size)
            pl.semaphore_signal(barrier, inc=1, device_id={axis: peer}, device_id_type=MESH)
    inputs = [
        pltpu.make_async_copy(src, dst, isem.at[i])
        for i, (src, dst) in enumerate(
            ((keys_hbm, keys_ref), (w_hbm, w_ref))
        )
    ]
    for copy in inputs:
        copy.start()
    tcopy = pltpu.make_async_copy(t_ref.at[y], traw, tsem)
    tcopy.start()
    own_q = pltpu.make_async_copy(q_ref.at[y], qx.at[y], lsem)
    own_q.start()
    for copy in inputs:
        copy.wait()
    live_here = 0
    for t in range(2):
        for j in range(SLOTS):
            live_here = live_here + jnp.where(chosen_s[t, j] >= 0, 1, 0)
    def invert(p):
        block = blocks_s[p]
        for t in range(2):
            at = 2 * SLOTS
            for j in range(SLOTS):
                at = jnp.where(chosen_s[t, j] == block, t * SLOTS + j, at)
            inv[t, p] = at

    loop(0, 2 * chips, invert)

    tcopy.wait()
    at_row = lax.broadcasted_iota(jnp.int32, (4 * BLOCK, BLOCK), 0)
    at_col = lax.broadcasted_iota(jnp.int32, (4 * BLOCK, BLOCK), 1)
    for q in range(NY):
        source = (at_col // QUARTER) * BLOCK + q * QUARTER + lax.rem(at_col, QUARTER)
        move = (at_row == source).astype(F32).astype(BF16)
        for m in range(4):
            got = jnp.dot(
                traw[:, m * 512 : (m + 1) * 512], move, preferred_element_type=F32
            )
            tgt[:, q * 512 + m * 128 : q * 512 + (m + 1) * 128] = got.astype(BF16)
    pl.semaphore_wait(barrier, nz + nx + NY + 2 - 4)

    def slot(core, cx, cz):
        return core * chips + cx * nz + cz

    here = slot(c, x, z)

    def z_copy(dz):
        return remote(
            keys_ref.at[:, mine, :], gath.at[here], zs.at[dz], zr.at[dz],
            {"z": lax.rem(z + dz, nz)},
        )

    def x_copy(dx, dz):
        at = slot(c, x, wrap(z - dz, nz))
        i = dx * nz + dz
        return remote(gath.at[at], gath.at[at], xs.at[i], xr.at[i], {"x": lax.rem(x + dx, nx)})

    def x_own(dx):
        return remote(
            keys_ref.at[:, mine, :], gath.at[here], xs.at[dx * nz], xr.at[dx * nz],
            {"x": lax.rem(x + dx, nx)},
        )

    def c_copy(dx, dz):
        at = slot(c, wrap(x - dx, nx), wrap(z - dz, nz))
        i = dx * nz + dz
        return remote(gath.at[at], gath.at[at], cs.at[i], cr.at[i], other)

    def c_own():
        return remote(keys_ref.at[:, mine, :], gath.at[here], cs.at[0], cr.at[0], other)

    def q_copy(i):
        peer = lax.rem(y + i, NY)
        return remote(q_ref.at[peer], qx.at[y], qs.at[i], qr.at[i], {"y": peer})

    def w_copy(i):
        peer = lax.rem(y + i, NY)
        lanes = pl.ds(pl.multiple_of((peer // 2) * BLOCK, BLOCK), BLOCK)
        return remote(w_ref.at[:, lanes], wx.at[y], ws.at[i], wr.at[i], {"y": peer})

    loop(1, nz, lambda k: z_copy(near(nz - k)).start())
    for dx in (2, 1, 3):
        x_own(dx).start()
    c_own().start()
    for i in (2, 1, 3):
        w_copy(i).start()
    for i in (2, 1, 3):
        q_copy(i).start()
    count_z.start(jnp.full((1, 128), live_here, jnp.int32).astype(F32))
    gath[here] = keys_ref[:, mine, :]
    wx[y] = w_ref[:, pl.ds(pl.multiple_of((y // 2) * BLOCK, BLOCK), BLOCK)]
    loop(2 * chips, 4 * chips, invert)

    def relay_z(k):
        dz = near(k)
        z_copy(dz).wait_recv()
        for dx in (2, 1, 3):
            x_copy(dx, dz).start()
        c_copy(0, dz).start()

    loop(1, nz, relay_z)
    count_x.start(count_z.finish())

    def relay_x(k):
        dz = near(k)
        for dx in (1, 3, 2):
            i = dx * nz + dz
            x_copy(dx, dz).wait_recv()
            c_copy(dx, dz).start()

    loop(0, nz, relay_x)
    count_c.start(count_x.finish())
    loop(0, chips, lambda i: c_copy(i // nz, lax.rem(i, nz)).wait_recv())

    for t in range(2):
        for j in range(SLOTS):
            block = jnp.maximum(chosen_s[t, j], 0)
            base = (block // 4) * 4
            pos = base
            for i in range(1, 4):
                pos = pos + jnp.where(blocks_s[base + i] == block, i, 0)
            device = pos // 2
            at = lax.rem(device, 2) * chips + device // 2
            sel[t, j] = gath[at, lax.rem(pos, 2)]

    def k_copy(i):
        peer = lax.rem(y + i, NY)
        return remote(sel.at[peer // 2], kx.at[y], ks.at[i], kr.at[i], {"y": peer})

    for i in (2, 1, 3):
        k_copy(i).start()
    kx[y] = sel[tile]

    for i in range(1, NY):
        w_copy(i).wait_recv()
    pick = (
        lax.broadcasted_iota(jnp.int32, (RG, BLOCK), 0) // HG + half
        == lax.broadcasted_iota(jnp.int32, (RG, BLOCK), 1)
    ).astype(F32).astype(BF16)
    head_lane = lax.rem(
        lax.broadcasted_iota(jnp.int32, (RG, BLOCK), 0), HG
    ) == lax.broadcasted_iota(jnp.int32, (RG, BLOCK), 1)
    ones = jnp.ones((BLOCK, BLOCK), BF16)
    for g in range(NY):
        wt = wx[g].astype(F32)
        wt = jnp.concatenate([wt, jnp.zeros((BLOCK - HG, BLOCK), F32)], axis=0).T.astype(BF16)
        row = jnp.dot(pick, wt, preferred_element_type=F32)
        row = jnp.where(head_lane, row, 0.0).astype(BF16)
        wb[g] = jnp.dot(row, ones, preferred_element_type=F32)


    own_q.wait()
    for i in range(1, NY):
        q_copy(i).wait_recv()
    for g in range(NY):
        for b in range(8):
            rows = slice(b * 128, (b + 1) * 128)
            wq = (qx[g, 8 * b : 8 * b + 8].reshape(128, DH).astype(F32) * wb[g, rows, :]).astype(BF16)
            qt[:, g * RG + b * 128 : g * RG + (b + 1) * 128] = wq.T
    count = count_c.finish() * float(BLOCK * BLOCK) - float(
        4 * chips * (BLOCK * BLOCK - BLOCK * (BLOCK + 1) // 2)
    )
    scale = (LOSS_SCALE * KEYS * SCORE_SCALE) / count

    def forward(k, part_of):
        at = wrap(y - near4(k), NY)
        cols = pl.ds(pl.multiple_of(at * 512 + part_of * 256, 256), 256)
        some = pl.ds(part_of * (SLOTS // 2), SLOTS // 2)
        kv = kx[at, some].reshape(256, DH)
        keys_t = jnp.concatenate([kv[:128].T, kv[128:].T], axis=1)
        for tb in range(4):
            rows = slice(tb * 256, (tb + 1) * 256)
            acc = None
            for g in range(NY):
                qv = qx[g, 16 * tb : 16 * tb + 16].reshape(256, DH)
                d = jnp.dot(qv, keys_t, preferred_element_type=F32)
                dots[g * RG + tb * 256 : g * RG + (tb + 1) * 256, cols] = d.astype(BF16)
                wv = wb[g, rows, :]
                term = jnp.maximum(d, 0.0) * jnp.concatenate([wv, wv], axis=1)
                acc = term if acc is None else acc + term
            sc[tb * 16 : (tb + 1) * 16, cols] = (
                jnp.sum(acc.reshape(16, 16, 256), axis=1) * SCORE_SCALE
            )

    def quarter(k):
        @pl.when(k > 0)
        def _():
            k_copy(near4(k)).wait_recv()

        loop(0, 2, lambda part_of: forward(k, part_of))

    loop(0, NY, quarter)

    row = lax.broadcasted_iota(jnp.int32, (ROWS, BLOCK), 0) + half
    col = lax.broadcasted_iota(jnp.int32, (ROWS, BLOCK), 1)
    group = col // QUARTER
    chosen_on = []
    for m in range(4):
        on = jnp.zeros((ROWS, BLOCK), jnp.int32)
        for u in range(4):
            one = jnp.where(chosen_s[tile, 4 * m + u] >= 0, 1, 0)
            on = jnp.where(group == u, jnp.full((ROWS, BLOCK), one, jnp.int32), on)
        chosen_on.append(on)

    def live(p):
        q, m = p // 4, p % 4
        on = chosen_on[m]
        if m == 0:
            on = jnp.where((group > 0) | (q * QUARTER + col <= row), on, 0)
        return on > 0

    def part(j):
        return slice(j * BLOCK, (j + 1) * BLOCK)

    top = None
    tsum = None
    for j in range(SLOTS):
        s = jnp.where(live(j), sc[:, part(j)], -1e30)
        t = jnp.where(live(j), tgt[:, part(j)].astype(F32), 0.0)
        top = s if top is None else jnp.maximum(top, s)
        tsum = t if tsum is None else tsum + t
    row_max = jnp.max(top, axis=1, keepdims=True)
    row_t = 1.0 / jnp.sum(tsum, axis=1, keepdims=True)
    esum = None
    for j in range(SLOTS):
        e = jnp.where(live(j), jnp.exp(jnp.where(live(j), sc[:, part(j)] - row_max, 0.0)), 0.0)
        gs[:, part(j)] = e
        esum = e if esum is None else esum + e
    norm = jnp.sum(esum, axis=1, keepdims=True)
    row_n = 1.0 / norm
    lse = row_max + jnp.log(norm)
    kl = None
    for j in range(SLOTS):
        on = live(j)
        prob = jnp.where(on, tgt[:, part(j)].astype(F32) * row_t, 0.0)
        term = jnp.where(
            on, prob * (jnp.log(jnp.where(on, prob, 1.0)) - sc[:, part(j)] + lse), 0.0
        )
        kl = term if kl is None else kl + term
        gs[:, part(j)] = gs[:, part(j)] * row_n - prob
    kl_row = jnp.sum(kl, axis=0, keepdims=True)
    loss_y.start(jnp.broadcast_to(jnp.sum(kl_row, axis=1, keepdims=True), (1, 128)))

    def d_copy(i):
        peer = lax.rem(y + i, NY)
        return remote(dks.at[peer], yrecv.at[y], ds_.at[i], dr.at[i], {"y": peer})

    def key_grad(k, part_of):
        at = lax.rem(y + near4(NY - 1 - k), NY)
        cols = pl.ds(pl.multiple_of(at * 512 + part_of * 256, 256), 256)
        got = None
        for tb in range(4):
            grad = jnp.concatenate(
                [
                    jnp.broadcast_to(gs[tb * 16 + u : tb * 16 + u + 1, cols], (HG, 256)).astype(BF16)
                    for u in range(16)
                ],
                axis=0,
            )
            for g in range(NY):
                rows = slice(g * RG + tb * 256, g * RG + (tb + 1) * 256)
                d = dots[rows, cols]
                d = jnp.where(d > 0, grad, jnp.zeros_like(grad))
                dots[rows, cols] = d
                term = jnp.dot(qt[:, rows], d, preferred_element_type=F32)
                got = term if got is None else got + term
        for u in range(2):
            block = (got[:, u * 128 : (u + 1) * 128].T * scale).astype(BF16)
            dks[at, pl.ds(part_of * 8 + u * 4, 4)] = block.reshape(4, QUARTER, DH)

    def key_quarter(k):
        loop(0, 2, lambda part_of: key_grad(k, part_of))

        @pl.when(k < NY - 1)
        def _():
            d_copy(near4(NY - 1 - k)).start()

    loop(0, NY, key_quarter)
    loss_z.start(loss_y.finish())

    def qg_copy(i):
        peer = lax.rem(y + i, NY)
        return remote(qg.at[peer], oq.at[y], gs_.at[i], gr.at[i], {"y": peer})

    def wg_copy(i):
        peer = lax.rem(y + i, NY)
        return remote(wg.at[peer], wgr.at[y], vs.at[i], vr.at[i], {"y": peer})

    def query_grad(i):
        g = lax.rem(y + i, NY)
        rows = pl.ds(pl.multiple_of(g * RG, RG), RG)
        a = jnp.dot(dots[rows, :], kx[...].reshape(KEYS, DH), preferred_element_type=F32) * scale
        qg[g] = (a * wb[g]).astype(BF16).reshape(ROWS, HG, DH)
        s = jnp.sum(a.reshape(ROWS, HG, DH) * qx[g].astype(F32), axis=2).T
        nil = jnp.zeros((HG, ROWS), F32)
        wg[g] = jnp.where(
            half == 0, jnp.concatenate([s, nil], axis=1), jnp.concatenate([nil, s], axis=1)
        )

    for i in (2, 1, 3):
        query_grad(i)
    loss_x.start(loss_z.finish())
    loop(1, nz, lambda dz: z_copy(dz).wait_send())
    c_own().wait_send()
    loop(1, chips, lambda i: c_copy(i // nz, lax.rem(i, nz)).wait_send())
    loop(nz, chips, lambda i: x_copy(i // nz, lax.rem(i, nz)).wait_send())
    for i in range(1, NY):
        q_copy(i).wait_send()
        w_copy(i).wait_send()
        k_copy(i).wait_send()
    for r in rows_of[:3]:
        r.drain()

    yrecv[y] = dks[y]
    table[2 * SLOTS] = jnp.zeros((QUARTER, DH), F32)
    for i in range(1, NY):
        d_copy(i).wait_recv()
    for i in (2, 1, 3):
        wg_copy(i).start()
        qg_copy(i).start()
    for t in range(2):
        def pair(j):
            table[t * SLOTS + j] = yrecv[2 * t, j].astype(F32) + yrecv[2 * t + 1, j].astype(F32)

        loop(0, SLOTS, pair)

    def dense(core, cx, dz, l):
        pos = slot(0, cx, lax.rem(z + dz, nz)) * 4 + core * 2 + l
        return table[inv[0, pos]] + table[inv[1, pos]]

    def e_copy(dz):
        return remote(dsend.at[dz], drecv.at[dz], es.at[dz], er.at[dz], other)

    def u_copy(dx, dz):
        to = lax.rem(x + dx, nx)
        i = dx * nz + dz
        return remote(pay.at[dz, to], xrecv.at[dx, dz], us.at[i], ur.at[i], {"x": to})

    def h_copy(dz):
        return remote(
            zsend.at[dz], zrecv.at[dz], hs.at[dz], hr.at[dz], {"z": lax.rem(z + dz, nz)}
        )

    def to_core(k):
        dz = near(nz - 1 - k)
        for cx in range(nx):
            for l in range(2):
                dsend[dz, cx, l] = dense(1 - c, cx, dz, l).astype(BF16)
        e_copy(dz).start()

    loop(0, nz, to_core)
    query_grad(0)
    own_o = pltpu.make_async_copy(qg.at[y], oq.at[y], osem)
    own_o.start()
    wgr[y] = wg[y]
    loss_c.start(loss_x.finish())

    def to_x(k):
        dz = near(nz - 1 - k)
        e_copy(dz).wait_recv()
        for cx in range(nx):
            for l in range(2):
                v = dense(c, cx, dz, l) + drecv[dz, cx, l].astype(F32)
                pay[dz, cx, l] = v.astype(BF16)
        for dx in (2, 1, 3):
            u_copy(dx, dz).start()

    loop(0, nz, to_x)
    loss = loss_c.finish() * float(KEYS) / count
    ol_v[...] = jnp.broadcast_to(loss, (8, 128))

    def x_total(dz):
        total = pay[dz, x].astype(F32)
        for dx in (1, 3, 2):
            u_copy(dx, dz).wait_recv()
            total = total + xrecv[dx, dz].astype(F32)
        return total

    def to_z(k):
        dz = near(nz - 1 - k)
        zsend[dz] = x_total(dz).astype(BF16)
        h_copy(dz).start()

    loop(0, nz - 1, to_z)
    fin[...] = x_total(0)
    def add_z(k):
        dz = near(k)
        h_copy(dz).wait_recv()
        fin[...] += zrecv[dz].astype(F32)

    loop(1, nz, add_z)

    def f_copy(i):
        return remote(
            fin_b, ok.at[:, mine, :], fs.at[i], fr.at[i], {"y": lax.rem(y + i, NY)}
        )

    fin_b[...] = fin[...].astype(BF16)
    for i in (2, 1, 3):
        f_copy(i).start()

    for i in range(1, NY):
        wg_copy(i).wait_recv()
    ow_v[:, 0:128] = wgr[0] + wgr[1]
    ow_v[:, 128:256] = wgr[2] + wgr[3]
    results = [
        pltpu.make_async_copy(src, dst, rsem.at[i])
        for i, (src, dst) in enumerate(((fin_b, ok.at[:, mine, :]), (ol_v, ol), (ow_v, ow)))
    ]
    for copy in results:
        copy.start()
    own_o.wait()
    loop(nz, chips, lambda i: u_copy(i // nz, lax.rem(i, nz)).wait_send())
    loop(0, nz, lambda dz: e_copy(dz).wait_send())
    loop(1, nz, lambda dz: h_copy(dz).wait_send())
    for r in rows_of[3:]:
        r.drain()
    for i in range(1, NY):
        d_copy(i).wait_send()
        wg_copy(i).wait_send()
        qg_copy(i).wait()
    for copy in results:
        copy.wait()
    for i in range(1, NY):
        f_copy(i).wait()


def finish_kernel(q_in, w_in, k_in, l_in, q_out, w_out, k_out, l_out):
    q_out[...] = q_in[...]
    w_out[...] = w_in[...]
    k_out[...] = k_in[...].astype(F32)
    l_out[0, 0] = l_in[0, 0]


VM = pl.BlockSpec(memory_space=pltpu.VMEM)
SM = pl.BlockSpec(memory_space=pltpu.SMEM)
ANY = pl.BlockSpec(memory_space=pl.ANY)


def shape(*dims_dtype):
    return jax.ShapeDtypeStruct(dims_dtype[:-1], dims_dtype[-1])


def local(nx, nz, queries, head_weights, keys, targets, chosen, tile_block):
    chips = nx * nz
    rows = NY * ROWS
    q4 = queries.reshape(NY, ROWS, HG, DH)
    v = pltpu.VMEM
    scratch = [
        v((HG, rows), BF16), v((2, BLOCK, DH), BF16),
        v((HG, rows), F32), v((8, 128), F32), v((2, QUARTER, DH), BF16), DMA((2,)), DMA((3,)),
        v((2 * chips, 2, QUARTER, DH), BF16),
        v((2, SLOTS, QUARTER, DH), BF16),
        v((NY, ROWS, HG, DH), BF16),
        v((NY, HG, BLOCK), BF16),
        v((NY, SLOTS, QUARTER, DH), BF16),
        v((NY, RG, DH), F32),
        v((DH, NY * RG), BF16),
        v((NY * RG, KEYS), BF16),
        v((ROWS, KEYS), F32),
        v((ROWS, KEYS), F32),
        v((ROWS, KEYS), BF16),
        v((ROWS, KEYS), BF16),
        v((NY, ROWS, HG, DH), BF16),
        v((NY, HG, BLOCK), F32),
        v((NY, HG, BLOCK), F32),
        pltpu.SMEM((2, 4 * chips), jnp.int32),
        v((NY, SLOTS, QUARTER, DH), BF16),
        v((NY, SLOTS, QUARTER, DH), BF16),
        v((2 * SLOTS + 1, QUARTER, DH), F32),
        v((nz, nx, 2, QUARTER, DH), BF16),
        v((nz, nx, 2, QUARTER, DH), BF16),
        v((nz, nx, 2, QUARTER, DH), BF16),
        v((nx, nz, 2, QUARTER, DH), BF16),
        v((nz, 2, QUARTER, DH), BF16),
        v((nz, 2, QUARTER, DH), BF16),
        v((2, QUARTER, DH), F32),
        DMA, DMA, DMA,
    ]
    for n in (NY, NY, nz, chips, chips, NY, NY, NY, NY, nz, chips, nz, NY):
        scratch += [DMA((n,)), DMA((n,))]
    for n in (nz, nx, 2, NY, nz, nx, 2):
        scratch += row_sum_scratch(n)
    oq, ow, ok, ol = pl.pallas_call(
        functools.partial(kernel, nx, nz),
        out_shape=[
            shape(NY, ROWS, HG, DH, BF16),
            shape(HG, rows, F32),
            shape(2, BLOCK, DH, BF16),
            shape(8, 128, F32),
        ],
        in_specs=[ANY, ANY, ANY, ANY, SM, SM],
        out_specs=[ANY] * 4,
        scratch_shapes=scratch,
        compiler_params=pltpu.CompilerParams(
            collective_id=0, has_side_effects=True, vmem_limit_bytes=60 * 1024 * 1024
        ),
        name="step",
    )(q4, head_weights.T, keys.reshape(2, BLOCK, DH), targets.reshape(NY, ROWS, KEYS), chosen, tile_block)
    oq, ow, ok, ol = pl.pallas_call(
        finish_kernel,
        out_shape=[
            shape(NY, ROWS, HG, DH, BF16),
            shape(HG, rows, F32),
            shape(2, BLOCK, DH, F32),
            shape(1, 1, F32),
        ],
        in_specs=[VM, VM, VM, VM],
        out_specs=[VM, VM, VM, SM],
        name="finish",
    )(oq, ow, ok, ol)
    return oq.reshape(rows, HG, DH), ow.T, ok.reshape(rows, DH), ol[0, 0]


def solution(mesh):
    nx, nz = 4, mesh.shape["seq"] // 8
    torus = Mesh(mesh.devices.reshape(nx, nz, 2, mesh.shape["head"]), ("x", "z", "c", "y"))
    in_specs = (P(SEQ, "y", None), P(SEQ, "y"), P(SEQ, None), P(SEQ, None), P(SEQ, None), P())
    out_specs = (P(SEQ, "y", None), P(SEQ, "y"), P(SEQ, None), P())
    return jax.shard_map(
        functools.partial(local, nx, nz),
        mesh=torus, in_specs=in_specs, out_specs=out_specs, check_vma=False,
    )
```

```python
import functools
import jax
import jax.numpy as jnp
from jax import lax
from jax.experimental import pallas as pl
from jax.experimental.pallas import tpu as pltpu
from jax.sharding import Mesh
from jax.sharding import PartitionSpec as P

BLOCK = 128
SLOTS = 16
KEYS = SLOTS * BLOCK
DH = 128
NY = 4
ROWS = 64
HG = 16
RG = ROWS * HG
QUARTER = BLOCK // NY
SEQ = ("x", "z", "c")
LOSS_SCALE = 4194304.0
SCORE_SCALE = DH ** (-0.5)
MESH = pl.DeviceIdType.MESH
F32 = jnp.float32
BF16 = jnp.bfloat16
DMA = pltpu.SemaphoreType.DMA


def remote(src, dst, send, recv, device):
    return pltpu.make_async_remote_copy(
        src_ref=src, dst_ref=dst, send_sem=send, recv_sem=recv,
        device_id=device, device_id_type=MESH,
    )


def loop(lo, hi, body):
    def step(i, carry):
        body(i)
        return carry

    lax.fori_loop(lo, hi, step, 0)


class RowSum:
    def __init__(self, axis, size, refs):
        self.axis, self.size = axis, size
        self.row, self.got, self.send, self.recv = refs

    def copy(self, i):
        peer = lax.rem(lax.axis_index(self.axis) + i, self.size)
        return remote(
            self.row, self.got.at[i], self.send.at[i], self.recv.at[i], {self.axis: peer}
        )

    def start(self, value):
        self.row[...] = value
        for i in range(1, self.size):
            self.copy(i).start()

    def finish(self):
        total = self.row[...]
        for i in range(1, self.size):
            self.copy(i).wait_recv()
            total = total + self.got[i]
        return total

    def drain(self):
        for i in range(1, self.size):
            self.copy(i).wait_send()


def row_sum_scratch(size):
    return [
        pltpu.VMEM((1, 128), F32), pltpu.VMEM((size, 1, 128), F32), DMA((size,)), DMA((size,)),
    ]


def kernel(
    nx, nz, q_ref, w_hbm, keys_hbm, t_ref, chosen_s, blocks_s,
    oq, ow, ok, ol,
    w_ref, keys_ref, ow_v, ol_v, fin_b, isem, rsem, gath, sel, qx, wx, kx, wb, qt, dots, sc, gs, traw, tgt, qg, wg, wgr, inv,
    dks, yrecv, table, dsend, drecv, pay, xrecv, zsend, zrecv, fin,
    tsem, lsem, osem, qs, qr, ws, wr, zs, zr, xs, xr, cs, cr, ks, kr,
    ds_, dr, gs_, gr, vs, vr, es, er, us, ur, hs, hr, fs, fr, *sums,
):
    chips = nx * nz
    x, z, c, y = (lax.axis_index(a) for a in ("x", "z", "c", "y"))
    other = {"c": 1 - c}
    tile = y // 2
    half = lax.rem(y, 2) * ROWS
    mine = pl.ds(pl.multiple_of(y * QUARTER, QUARTER), QUARTER)
    sizes = [("z", nz), ("x", nx), ("c", 2), ("y", NY), ("z", nz), ("x", nx), ("c", 2)]
    rows_of = [
        RowSum(a, n, sums[4 * i : 4 * i + 4]) for i, (a, n) in enumerate(sizes)
    ]
    count_z, count_x, count_c, loss_y, loss_z, loss_x, loss_c = rows_of

    def near(k):
        odd = lax.rem(k, 2)
        return odd * ((k + 1) // 2) + (1 - odd) * lax.rem(nz - k // 2, nz)

    def near4(k):
        odd = lax.rem(k, 2)
        return odd * ((k + 1) // 2) + (1 - odd) * lax.rem(NY - k // 2, NY)

    def wrap(v, n):
        return lax.rem(v + n, n)

    barrier = pltpu.get_barrier_semaphore()
    for axis, size in (("z", nz), ("x", nx), ("y", NY), ("c", 2)):
        for i in range(1, size):
            peer = lax.rem(lax.axis_index(axis) + i, size)
            pl.semaphore_signal(barrier, inc=1, device_id={axis: peer}, device_id_type=MESH)
    inputs = [
        pltpu.make_async_copy(src, dst, isem.at[i])
        for i, (src, dst) in enumerate(
            ((keys_hbm, keys_ref), (w_hbm, w_ref))
        )
    ]
    for copy in inputs:
        copy.start()
    tcopy = pltpu.make_async_copy(t_ref.at[y], traw, tsem)
    tcopy.start()
    own_q = pltpu.make_async_copy(q_ref.at[y], qx.at[y], lsem)
    own_q.start()
    for copy in inputs:
        copy.wait()
    live_here = 0
    for t in range(2):
        for j in range(SLOTS):
            live_here = live_here + jnp.where(chosen_s[t, j] >= 0, 1, 0)
    def invert(p):
        block = blocks_s[p]
        for t in range(2):
            at = 2 * SLOTS
            for j in range(SLOTS):
                at = jnp.where(chosen_s[t, j] == block, t * SLOTS + j, at)
            inv[t, p] = at

    loop(0, 2 * chips, invert)

    tcopy.wait()
    at_row = lax.broadcasted_iota(jnp.int32, (4 * BLOCK, BLOCK), 0)
    at_col = lax.broadcasted_iota(jnp.int32, (4 * BLOCK, BLOCK), 1)
    for q in range(NY):
        source = (at_col // QUARTER) * BLOCK + q * QUARTER + lax.rem(at_col, QUARTER)
        move = (at_row == source).astype(F32).astype(BF16)
        for m in range(4):
            got = jnp.dot(
                traw[:, m * 512 : (m + 1) * 512], move, preferred_element_type=F32
            )
            tgt[:, q * 512 + m * 128 : q * 512 + (m + 1) * 128] = got.astype(BF16)
    pl.semaphore_wait(barrier, nz + nx + NY + 2 - 4)

    def slot(core, cx, cz):
        return core * chips + cx * nz + cz

    here = slot(c, x, z)

    def z_copy(dz):
        return remote(
            keys_ref.at[:, mine, :], gath.at[here], zs.at[dz], zr.at[dz],
            {"z": lax.rem(z + dz, nz)},
        )

    def x_copy(dx, dz):
        at = slot(c, x, wrap(z - dz, nz))
        i = dx * nz + dz
        return remote(gath.at[at], gath.at[at], xs.at[i], xr.at[i], {"x": lax.rem(x + dx, nx)})

    def x_own(dx):
        return remote(
            keys_ref.at[:, mine, :], gath.at[here], xs.at[dx * nz], xr.at[dx * nz],
            {"x": lax.rem(x + dx, nx)},
        )

    def c_copy(dx, dz):
        at = slot(c, wrap(x - dx, nx), wrap(z - dz, nz))
        i = dx * nz + dz
        return remote(gath.at[at], gath.at[at], cs.at[i], cr.at[i], other)

    def c_own():
        return remote(keys_ref.at[:, mine, :], gath.at[here], cs.at[0], cr.at[0], other)

    def q_copy(i):
        peer = lax.rem(y + i, NY)
        return remote(q_ref.at[peer], qx.at[y], qs.at[i], qr.at[i], {"y": peer})

    def w_copy(i):
        peer = lax.rem(y + i, NY)
        lanes = pl.ds(pl.multiple_of((peer // 2) * BLOCK, BLOCK), BLOCK)
        return remote(w_ref.at[:, lanes], wx.at[y], ws.at[i], wr.at[i], {"y": peer})

    loop(1, nz, lambda k: z_copy(near(nz - k)).start())
    for dx in (2, 1, 3):
        x_own(dx).start()
    c_own().start()
    for i in (2, 1, 3):
        w_copy(i).start()
    for i in (2, 1, 3):
        q_copy(i).start()
    count_z.start(jnp.full((1, 128), live_here, jnp.int32).astype(F32))
    gath[here] = keys_ref[:, mine, :]
    wx[y] = w_ref[:, pl.ds(pl.multiple_of((y // 2) * BLOCK, BLOCK), BLOCK)]
    loop(2 * chips, 4 * chips, invert)

    def relay_z(k):
        dz = near(k)
        z_copy(dz).wait_recv()
        for dx in (2, 1, 3):
            x_copy(dx, dz).start()
        c_copy(0, dz).start()

    loop(1, nz, relay_z)
    count_x.start(count_z.finish())

    def relay_x(k):
        dz = near(k)
        for dx in (1, 3, 2):
            i = dx * nz + dz
            x_copy(dx, dz).wait_recv()
            c_copy(dx, dz).start()

    loop(0, nz, relay_x)
    count_c.start(count_x.finish())
    loop(0, chips, lambda i: c_copy(i // nz, lax.rem(i, nz)).wait_recv())

    for t in range(2):
        for j in range(SLOTS):
            block = jnp.maximum(chosen_s[t, j], 0)
            base = (block // 4) * 4
            pos = base
            for i in range(1, 4):
                pos = pos + jnp.where(blocks_s[base + i] == block, i, 0)
            device = pos // 2
            at = lax.rem(device, 2) * chips + device // 2
            sel[t, j] = gath[at, lax.rem(pos, 2)]

    def k_copy(i):
        peer = lax.rem(y + i, NY)
        return remote(sel.at[peer // 2], kx.at[y], ks.at[i], kr.at[i], {"y": peer})

    for i in (1, 3, 2):
        k_copy(i).start()
    kx[y] = sel[tile]

    for i in range(1, NY):
        w_copy(i).wait_recv()
    pick = (
        lax.broadcasted_iota(jnp.int32, (RG, BLOCK), 0) // HG + half
        == lax.broadcasted_iota(jnp.int32, (RG, BLOCK), 1)
    ).astype(F32).astype(BF16)
    head_lane = lax.rem(
        lax.broadcasted_iota(jnp.int32, (RG, BLOCK), 0), HG
    ) == lax.broadcasted_iota(jnp.int32, (RG, BLOCK), 1)
    ones = jnp.ones((BLOCK, BLOCK), BF16)
    for g in range(NY):
        wt = wx[g].astype(F32)
        wt = jnp.concatenate([wt, jnp.zeros((BLOCK - HG, BLOCK), F32)], axis=0).T.astype(BF16)
        row = jnp.dot(pick, wt, preferred_element_type=F32)
        row = jnp.where(head_lane, row, 0.0).astype(BF16)
        wb[g] = jnp.dot(row, ones, preferred_element_type=F32)


    own_q.wait()
    for i in range(1, NY):
        q_copy(i).wait_recv()
    for g in range(NY):
        for b in range(8):
            rows = slice(b * 128, (b + 1) * 128)
            wq = (qx[g, 8 * b : 8 * b + 8].reshape(128, DH).astype(F32) * wb[g, rows, :]).astype(BF16)
            qt[:, g * RG + b * 128 : g * RG + (b + 1) * 128] = wq.T
    count = count_c.finish() * float(BLOCK * BLOCK) - float(
        4 * chips * (BLOCK * BLOCK - BLOCK * (BLOCK + 1) // 2)
    )
    scale = (LOSS_SCALE * KEYS * SCORE_SCALE) / count

    def forward(k, part_of):
        at = wrap(y - near4(k), NY)
        cols = pl.ds(pl.multiple_of(at * 512 + part_of * 256, 256), 256)
        some = pl.ds(part_of * (SLOTS // 2), SLOTS // 2)
        kv = kx[at, some].reshape(256, DH)
        keys_t = jnp.concatenate([kv[:128].T, kv[128:].T], axis=1)
        for tb in range(4):
            rows = slice(tb * 256, (tb + 1) * 256)
            acc = None
            for g in range(NY):
                qv = qx[g, 16 * tb : 16 * tb + 16].reshape(256, DH)
                d = jnp.dot(qv, keys_t, preferred_element_type=F32)
                dots[g * RG + tb * 256 : g * RG + (tb + 1) * 256, cols] = d.astype(BF16)
                wv = wb[g, rows, :]
                term = jnp.maximum(d, 0.0) * jnp.concatenate([wv, wv], axis=1)
                acc = term if acc is None else acc + term
            sc[tb * 16 : (tb + 1) * 16, cols] = (
                jnp.sum(acc.reshape(16, 16, 256), axis=1) * SCORE_SCALE
            )

    def quarter(k):
        @pl.when(k > 0)
        def _():
            k_copy(near4(k)).wait_recv()

        loop(0, 2, lambda part_of: forward(k, part_of))

    loop(0, NY, quarter)

    row = lax.broadcasted_iota(jnp.int32, (ROWS, BLOCK), 0) + half
    col = lax.broadcasted_iota(jnp.int32, (ROWS, BLOCK), 1)
    group = col // QUARTER
    chosen_on = []
    for m in range(4):
        on = jnp.zeros((ROWS, BLOCK), jnp.int32)
        for u in range(4):
            one = jnp.where(chosen_s[tile, 4 * m + u] >= 0, 1, 0)
            on = jnp.where(group == u, jnp.full((ROWS, BLOCK), one, jnp.int32), on)
        chosen_on.append(on)

    def live(p):
        q, m = p // 4, p % 4
        on = chosen_on[m]
        if m == 0:
            on = jnp.where((group > 0) | (q * QUARTER + col <= row), on, 0)
        return on > 0

    def part(j):
        return slice(j * BLOCK, (j + 1) * BLOCK)

    top = None
    tsum = None
    for j in range(SLOTS):
        s = jnp.where(live(j), sc[:, part(j)], -1e30)
        t = jnp.where(live(j), tgt[:, part(j)].astype(F32), 0.0)
        top = s if top is None else jnp.maximum(top, s)
        tsum = t if tsum is None else tsum + t
    row_max = jnp.max(top, axis=1, keepdims=True)
    row_t = 1.0 / jnp.sum(tsum, axis=1, keepdims=True)
    esum = None
    for j in range(SLOTS):
        e = jnp.where(live(j), jnp.exp(jnp.where(live(j), sc[:, part(j)] - row_max, 0.0)), 0.0)
        gs[:, part(j)] = e
        esum = e if esum is None else esum + e
    norm = jnp.sum(esum, axis=1, keepdims=True)
    row_n = 1.0 / norm
    lse = row_max + jnp.log(norm)
    kl = None
    for j in range(SLOTS):
        on = live(j)
        prob = jnp.where(on, tgt[:, part(j)].astype(F32) * row_t, 0.0)
        term = jnp.where(
            on, prob * (jnp.log(jnp.where(on, prob, 1.0)) - sc[:, part(j)] + lse), 0.0
        )
        kl = term if kl is None else kl + term
        gs[:, part(j)] = gs[:, part(j)] * row_n - prob
    kl_row = jnp.sum(kl, axis=0, keepdims=True)
    loss_y.start(jnp.broadcast_to(jnp.sum(kl_row, axis=1, keepdims=True), (1, 128)))

    def d_copy(i):
        peer = lax.rem(y + i, NY)
        return remote(dks.at[peer], yrecv.at[y], ds_.at[i], dr.at[i], {"y": peer})

    def key_grad(k, part_of):
        at = lax.rem(y + near4(NY - 1 - k), NY)
        cols = pl.ds(pl.multiple_of(at * 512 + part_of * 256, 256), 256)
        got = None
        for tb in range(4):
            grad = jnp.concatenate(
                [
                    jnp.broadcast_to(gs[tb * 16 + u : tb * 16 + u + 1, cols], (HG, 256)).astype(BF16)
                    for u in range(16)
                ],
                axis=0,
            )
            for g in range(NY):
                rows = slice(g * RG + tb * 256, g * RG + (tb + 1) * 256)
                d = dots[rows, cols]
                d = jnp.where(d > 0, grad, jnp.zeros_like(grad))
                dots[rows, cols] = d
                term = jnp.dot(qt[:, rows], d, preferred_element_type=F32)
                got = term if got is None else got + term
        for u in range(2):
            block = (got[:, u * 128 : (u + 1) * 128].T * scale).astype(BF16)
            dks[at, pl.ds(part_of * 8 + u * 4, 4)] = block.reshape(4, QUARTER, DH)

    def key_quarter(k):
        loop(0, 2, lambda part_of: key_grad(k, part_of))

        @pl.when(k < NY - 1)
        def _():
            d_copy(near4(NY - 1 - k)).start()

    loop(0, NY, key_quarter)
    loss_z.start(loss_y.finish())

    def qg_copy(i):
        peer = lax.rem(y + i, NY)
        return remote(qg.at[peer], oq.at[y], gs_.at[i], gr.at[i], {"y": peer})

    def wg_copy(i):
        peer = lax.rem(y + i, NY)
        return remote(wg.at[peer], wgr.at[y], vs.at[i], vr.at[i], {"y": peer})

    def query_grad(i):
        g = lax.rem(y + i, NY)
        rows = pl.ds(pl.multiple_of(g * RG, RG), RG)
        a = jnp.dot(dots[rows, :], kx[...].reshape(KEYS, DH), preferred_element_type=F32) * scale
        qg[g] = (a * wb[g]).astype(BF16).reshape(ROWS, HG, DH)
        s = jnp.sum(a.reshape(ROWS, HG, DH) * qx[g].astype(F32), axis=2).T
        nil = jnp.zeros((HG, ROWS), F32)
        wg[g] = jnp.where(
            half == 0, jnp.concatenate([s, nil], axis=1), jnp.concatenate([nil, s], axis=1)
        )

    for i in (2, 1, 3, 0):
        query_grad(i)
    loss_x.start(loss_z.finish())
    loop(1, nz, lambda dz: z_copy(dz).wait_send())
    c_own().wait_send()
    loop(1, chips, lambda i: c_copy(i // nz, lax.rem(i, nz)).wait_send())
    loop(nz, chips, lambda i: x_copy(i // nz, lax.rem(i, nz)).wait_send())
    for i in range(1, NY):
        q_copy(i).wait_send()
        w_copy(i).wait_send()
        k_copy(i).wait_send()
    for r in rows_of[:3]:
        r.drain()

    yrecv[y] = dks[y]
    table[2 * SLOTS] = jnp.zeros((QUARTER, DH), F32)
    for i in range(1, NY):
        d_copy(i).wait_recv()
    for i in (2, 1, 3):
        wg_copy(i).start()
        qg_copy(i).start()
    for t in range(2):
        def pair(j):
            table[t * SLOTS + j] = yrecv[2 * t, j].astype(F32) + yrecv[2 * t + 1, j].astype(F32)

        loop(0, SLOTS, pair)

    def dense(core, cx, dz, l):
        pos = slot(0, cx, lax.rem(z + dz, nz)) * 4 + core * 2 + l
        return table[inv[0, pos]] + table[inv[1, pos]]

    def e_copy(dz):
        return remote(dsend.at[dz], drecv.at[dz], es.at[dz], er.at[dz], other)

    def u_copy(dx, dz):
        to = lax.rem(x + dx, nx)
        i = dx * nz + dz
        return remote(pay.at[dz, to], xrecv.at[dx, dz], us.at[i], ur.at[i], {"x": to})

    def h_copy(dz):
        return remote(
            zsend.at[dz], zrecv.at[dz], hs.at[dz], hr.at[dz], {"z": lax.rem(z + dz, nz)}
        )

    def to_core(k):
        dz = near(nz - 1 - k)
        for cx in range(nx):
            for l in range(2):
                dsend[dz, cx, l] = dense(1 - c, cx, dz, l).astype(BF16)
        e_copy(dz).start()

    loop(0, nz, to_core)
    own_o = pltpu.make_async_copy(qg.at[y], oq.at[y], osem)
    own_o.start()
    wgr[y] = wg[y]
    loss_c.start(loss_x.finish())

    def to_x(k):
        dz = near(nz - 1 - k)
        e_copy(dz).wait_recv()
        for cx in range(nx):
            for l in range(2):
                v = dense(c, cx, dz, l) + drecv[dz, cx, l].astype(F32)
                pay[dz, cx, l] = v.astype(BF16)
        for dx in (2, 1, 3):
            u_copy(dx, dz).start()

    loop(0, nz, to_x)
    loss = loss_c.finish() * float(KEYS) / count
    ol_v[...] = jnp.broadcast_to(loss, (8, 128))

    def x_total(dz):
        total = pay[dz, x].astype(F32)
        for dx in (1, 3, 2):
            u_copy(dx, dz).wait_recv()
            total = total + xrecv[dx, dz].astype(F32)
        return total

    def to_z(k):
        dz = near(nz - 1 - k)
        zsend[dz] = x_total(dz).astype(BF16)
        h_copy(dz).start()

    loop(0, nz - 1, to_z)
    fin[...] = x_total(0)
    def add_z(k):
        dz = near(k)
        h_copy(dz).wait_recv()
        fin[...] += zrecv[dz].astype(F32)

    loop(1, nz, add_z)

    def f_copy(i):
        return remote(
            fin_b, ok.at[:, mine, :], fs.at[i], fr.at[i], {"y": lax.rem(y + i, NY)}
        )

    fin_b[...] = fin[...].astype(BF16)
    for i in (2, 1, 3):
        f_copy(i).start()

    for i in range(1, NY):
        wg_copy(i).wait_recv()
    ow_v[:, 0:128] = wgr[0] + wgr[1]
    ow_v[:, 128:256] = wgr[2] + wgr[3]
    results = [
        pltpu.make_async_copy(src, dst, rsem.at[i])
        for i, (src, dst) in enumerate(((fin_b, ok.at[:, mine, :]), (ol_v, ol), (ow_v, ow)))
    ]
    for copy in results:
        copy.start()
    own_o.wait()
    loop(nz, chips, lambda i: u_copy(i // nz, lax.rem(i, nz)).wait_send())
    loop(0, nz, lambda dz: e_copy(dz).wait_send())
    loop(1, nz, lambda dz: h_copy(dz).wait_send())
    for r in rows_of[3:]:
        r.drain()
    for i in range(1, NY):
        d_copy(i).wait_send()
        wg_copy(i).wait_send()
        qg_copy(i).wait()
    for copy in results:
        copy.wait()
    for i in range(1, NY):
        f_copy(i).wait()


def finish_kernel(q_in, w_in, k_in, l_in, q_out, w_out, k_out, l_out):
    q_out[...] = q_in[...]
    w_out[...] = w_in[...]
    k_out[...] = k_in[...].astype(F32)
    l_out[0, 0] = l_in[0, 0]


VM = pl.BlockSpec(memory_space=pltpu.VMEM)
SM = pl.BlockSpec(memory_space=pltpu.SMEM)
ANY = pl.BlockSpec(memory_space=pl.ANY)


def shape(*dims_dtype):
    return jax.ShapeDtypeStruct(dims_dtype[:-1], dims_dtype[-1])


def local(nx, nz, queries, head_weights, keys, targets, chosen, tile_block):
    chips = nx * nz
    rows = NY * ROWS
    q4 = queries.reshape(NY, ROWS, HG, DH)
    v = pltpu.VMEM
    scratch = [
        v((HG, rows), BF16), v((2, BLOCK, DH), BF16),
        v((HG, rows), F32), v((8, 128), F32), v((2, QUARTER, DH), BF16), DMA((2,)), DMA((3,)),
        v((2 * chips, 2, QUARTER, DH), BF16),
        v((2, SLOTS, QUARTER, DH), BF16),
        v((NY, ROWS, HG, DH), BF16),
        v((NY, HG, BLOCK), BF16),
        v((NY, SLOTS, QUARTER, DH), BF16),
        v((NY, RG, DH), F32),
        v((DH, NY * RG), BF16),
        v((NY * RG, KEYS), BF16),
        v((ROWS, KEYS), F32),
        v((ROWS, KEYS), F32),
        v((ROWS, KEYS), BF16),
        v((ROWS, KEYS), BF16),
        v((NY, ROWS, HG, DH), BF16),
        v((NY, HG, BLOCK), F32),
        v((NY, HG, BLOCK), F32),
        pltpu.SMEM((2, 4 * chips), jnp.int32),
        v((NY, SLOTS, QUARTER, DH), BF16),
        v((NY, SLOTS, QUARTER, DH), BF16),
        v((2 * SLOTS + 1, QUARTER, DH), F32),
        v((nz, nx, 2, QUARTER, DH), BF16),
        v((nz, nx, 2, QUARTER, DH), BF16),
        v((nz, nx, 2, QUARTER, DH), BF16),
        v((nx, nz, 2, QUARTER, DH), BF16),
        v((nz, 2, QUARTER, DH), BF16),
        v((nz, 2, QUARTER, DH), BF16),
        v((2, QUARTER, DH), F32),
        DMA, DMA, DMA,
    ]
    for n in (NY, NY, nz, chips, chips, NY, NY, NY, NY, nz, chips, nz, NY):
        scratch += [DMA((n,)), DMA((n,))]
    for n in (nz, nx, 2, NY, nz, nx, 2):
        scratch += row_sum_scratch(n)
    oq, ow, ok, ol = pl.pallas_call(
        functools.partial(kernel, nx, nz),
        out_shape=[
            shape(NY, ROWS, HG, DH, BF16),
            shape(HG, rows, F32),
            shape(2, BLOCK, DH, BF16),
            shape(8, 128, F32),
        ],
        in_specs=[ANY, ANY, ANY, ANY, SM, SM],
        out_specs=[ANY] * 4,
        scratch_shapes=scratch,
        compiler_params=pltpu.CompilerParams(
            collective_id=0, has_side_effects=True, vmem_limit_bytes=60 * 1024 * 1024
        ),
        name="step",
    )(q4, head_weights.T, keys.reshape(2, BLOCK, DH), targets.reshape(NY, ROWS, KEYS), chosen, tile_block)
    oq, ow, ok, ol = pl.pallas_call(
        finish_kernel,
        out_shape=[
            shape(NY, ROWS, HG, DH, BF16),
            shape(HG, rows, F32),
            shape(2, BLOCK, DH, F32),
            shape(1, 1, F32),
        ],
        in_specs=[VM, VM, VM, VM],
        out_specs=[VM, VM, VM, SM],
        name="finish",
    )(oq, ow, ok, ol)
    return oq.reshape(rows, HG, DH), ow.T, ok.reshape(rows, DH), ol[0, 0]


def solution(mesh):
    nx, nz = 4, mesh.shape["seq"] // 8
    torus = Mesh(mesh.devices.reshape(nx, nz, 2, mesh.shape["head"]), ("x", "z", "c", "y"))
    in_specs = (P(SEQ, "y", None), P(SEQ, "y"), P(SEQ, None), P(SEQ, None), P(SEQ, None), P())
    out_specs = (P(SEQ, "y", None), P(SEQ, "y"), P(SEQ, None), P())
    return jax.shard_map(
        functools.partial(local, nx, nz),
        mesh=torus, in_specs=in_specs, out_specs=out_specs, check_vma=False,
    )
```

```python
import functools
import jax
import jax.numpy as jnp
from jax import lax
from jax.experimental import pallas as pl
from jax.experimental.pallas import tpu as pltpu
from jax.sharding import Mesh
from jax.sharding import PartitionSpec as P

BLOCK = 128
SLOTS = 16
KEYS = SLOTS * BLOCK
DH = 128
NY = 4
ROWS = 64
HG = 16
RG = ROWS * HG
QUARTER = BLOCK // NY
SEQ = ("x", "z", "c")
LOSS_SCALE = 4194304.0
SCORE_SCALE = DH ** (-0.5)
MESH = pl.DeviceIdType.MESH
F32 = jnp.float32
BF16 = jnp.bfloat16
DMA = pltpu.SemaphoreType.DMA


def remote(src, dst, send, recv, device):
    return pltpu.make_async_remote_copy(
        src_ref=src, dst_ref=dst, send_sem=send, recv_sem=recv,
        device_id=device, device_id_type=MESH,
    )


def loop(lo, hi, body):
    def step(i, carry):
        body(i)
        return carry

    lax.fori_loop(lo, hi, step, 0)


class RowSum:
    def __init__(self, axis, size, refs):
        self.axis, self.size = axis, size
        self.row, self.got, self.send, self.recv = refs

    def copy(self, i):
        peer = lax.rem(lax.axis_index(self.axis) + i, self.size)
        return remote(
            self.row, self.got.at[i], self.send.at[i], self.recv.at[i], {self.axis: peer}
        )

    def start(self, value):
        self.row[...] = value
        for i in range(1, self.size):
            self.copy(i).start()

    def finish(self):
        total = self.row[...]
        for i in range(1, self.size):
            self.copy(i).wait_recv()
            total = total + self.got[i]
        return total

    def drain(self):
        for i in range(1, self.size):
            self.copy(i).wait_send()


def row_sum_scratch(size):
    return [
        pltpu.VMEM((1, 128), F32), pltpu.VMEM((size, 1, 128), F32), DMA((size,)), DMA((size,)),
    ]


def kernel(
    nx, nz, q_ref, w_hbm, keys_hbm, t_ref, chosen_s, blocks_s,
    oq, ow, ok, ol,
    w_ref, keys_ref, ow_v, ol_v, fin_b, isem, rsem, gath, sel, qx, wx, kx, wb, qt, dots, sc, gs, traw, tgt, qg, wg, wgr, inv,
    dks, yrecv, table, dsend, drecv, pay, xrecv, zsend, zrecv, fin,
    tsem, lsem, osem, qs, qr, ws, wr, zs, zr, xs, xr, cs, cr, ks, kr,
    ds_, dr, gs_, gr, vs, vr, es, er, us, ur, hs, hr, fs, fr, *sums,
):
    chips = nx * nz
    x, z, c, y = (lax.axis_index(a) for a in ("x", "z", "c", "y"))
    other = {"c": 1 - c}
    tile = y // 2
    half = lax.rem(y, 2) * ROWS
    mine = pl.ds(pl.multiple_of(y * QUARTER, QUARTER), QUARTER)
    sizes = [("z", nz), ("x", nx), ("c", 2), ("y", NY), ("z", nz), ("x", nx), ("c", 2)]
    rows_of = [
        RowSum(a, n, sums[4 * i : 4 * i + 4]) for i, (a, n) in enumerate(sizes)
    ]
    count_z, count_x, count_c, loss_y, loss_z, loss_x, loss_c = rows_of

    def near(k):
        odd = lax.rem(k, 2)
        return odd * ((k + 1) // 2) + (1 - odd) * lax.rem(nz - k // 2, nz)

    def near4(k):
        odd = lax.rem(k, 2)
        return odd * ((k + 1) // 2) + (1 - odd) * lax.rem(NY - k // 2, NY)

    def wrap(v, n):
        return lax.rem(v + n, n)

    barrier = pltpu.get_barrier_semaphore()
    for axis, size in (("z", nz), ("x", nx), ("y", NY), ("c", 2)):
        for i in range(1, size):
            peer = lax.rem(lax.axis_index(axis) + i, size)
            pl.semaphore_signal(barrier, inc=1, device_id={axis: peer}, device_id_type=MESH)
    inputs = [
        pltpu.make_async_copy(src, dst, isem.at[i])
        for i, (src, dst) in enumerate(
            ((keys_hbm, keys_ref), (w_hbm, w_ref))
        )
    ]
    for copy in inputs:
        copy.start()
    tcopy = pltpu.make_async_copy(t_ref.at[y], traw, tsem)
    tcopy.start()
    own_q = pltpu.make_async_copy(q_ref.at[y], qx.at[y], lsem)
    own_q.start()
    for copy in inputs:
        copy.wait()
    live_here = 0
    for t in range(2):
        for j in range(SLOTS):
            live_here = live_here + jnp.where(chosen_s[t, j] >= 0, 1, 0)
    def invert(p):
        block = blocks_s[p]
        for t in range(2):
            at = 2 * SLOTS
            for j in range(SLOTS):
                at = jnp.where(chosen_s[t, j] == block, t * SLOTS + j, at)
            inv[t, p] = at

    loop(0, 2 * chips, invert)

    tcopy.wait()
    at_row = lax.broadcasted_iota(jnp.int32, (4 * BLOCK, BLOCK), 0)
    at_col = lax.broadcasted_iota(jnp.int32, (4 * BLOCK, BLOCK), 1)
    for q in range(NY):
        source = (at_col // QUARTER) * BLOCK + q * QUARTER + lax.rem(at_col, QUARTER)
        move = (at_row == source).astype(F32).astype(BF16)
        for m in range(4):
            got = jnp.dot(
                traw[:, m * 512 : (m + 1) * 512], move, preferred_element_type=F32
            )
            tgt[:, q * 512 + m * 128 : q * 512 + (m + 1) * 128] = got.astype(BF16)
    pl.semaphore_wait(barrier, nz + nx + NY + 2 - 4)

    def slot(core, cx, cz):
        return core * chips + cx * nz + cz

    def held(core, cx, cz):
        return core * chips + cz * nx + cx

    here = held(c, x, z)

    def z_copy(dz):
        return remote(
            keys_ref.at[:, mine, :], gath.at[here], zs.at[dz], zr.at[dz],
            {"z": lax.rem(z + dz, nz)},
        )

    def x_copy(dx, dz):
        at = held(c, x, wrap(z - dz, nz))
        i = dx * nz + dz
        return remote(gath.at[at], gath.at[at], xs.at[i], xr.at[i], {"x": lax.rem(x + dx, nx)})

    def x_own(dx):
        return remote(
            keys_ref.at[:, mine, :], gath.at[here], xs.at[dx * nz], xr.at[dx * nz],
            {"x": lax.rem(x + dx, nx)},
        )

    def c_copy(dz):
        some = pl.ds(held(c, 0, wrap(z - dz, nz)), nx)
        return remote(gath.at[some], gath.at[some], cs.at[dz], cr.at[dz], other)

    def q_copy(i):
        peer = lax.rem(y + i, NY)
        return remote(q_ref.at[peer], qx.at[y], qs.at[i], qr.at[i], {"y": peer})

    def w_copy(i):
        peer = lax.rem(y + i, NY)
        lanes = pl.ds(pl.multiple_of((peer // 2) * BLOCK, BLOCK), BLOCK)
        return remote(w_ref.at[:, lanes], wx.at[y], ws.at[i], wr.at[i], {"y": peer})

    loop(1, nz, lambda k: z_copy(near(nz - k)).start())
    for dx in (2, 1, 3):
        x_own(dx).start()
    for i in (2, 1, 3):
        w_copy(i).start()
    for i in (2, 1, 3):
        q_copy(i).start()
    count_z.start(jnp.full((1, 128), live_here, jnp.int32).astype(F32))
    gath[here] = keys_ref[:, mine, :]
    wx[y] = w_ref[:, pl.ds(pl.multiple_of((y // 2) * BLOCK, BLOCK), BLOCK)]
    loop(2 * chips, 4 * chips, invert)

    def relay_z(k):
        dz = near(k)
        z_copy(dz).wait_recv()
        for dx in (2, 1, 3):
            x_copy(dx, dz).start()

    loop(1, nz, relay_z)
    count_x.start(count_z.finish())

    def relay_x(k):
        dz = near(k)
        for dx in (1, 3, 2):
            x_copy(dx, dz).wait_recv()
        c_copy(dz).start()

    loop(0, nz, relay_x)
    count_c.start(count_x.finish())
    loop(0, nz, lambda dz: c_copy(dz).wait_recv())

    for t in range(2):
        for j in range(SLOTS):
            block = jnp.maximum(chosen_s[t, j], 0)
            base = (block // 4) * 4
            pos = base
            for i in range(1, 4):
                pos = pos + jnp.where(blocks_s[base + i] == block, i, 0)
            device = pos // 2
            at = held(lax.rem(device, 2), device // (2 * nz), lax.rem(device // 2, nz))
            sel[t, j] = gath[at, lax.rem(pos, 2)]

    def k_copy(i):
        peer = lax.rem(y + i, NY)
        return remote(sel.at[peer // 2], kx.at[y], ks.at[i], kr.at[i], {"y": peer})

    for i in (1, 3, 2):
        k_copy(i).start()
    kx[y] = sel[tile]

    for i in range(1, NY):
        w_copy(i).wait_recv()
    pick = (
        lax.broadcasted_iota(jnp.int32, (RG, BLOCK), 0) // HG + half
        == lax.broadcasted_iota(jnp.int32, (RG, BLOCK), 1)
    ).astype(F32).astype(BF16)
    head_lane = lax.rem(
        lax.broadcasted_iota(jnp.int32, (RG, BLOCK), 0), HG
    ) == lax.broadcasted_iota(jnp.int32, (RG, BLOCK), 1)
    ones = jnp.ones((BLOCK, BLOCK), BF16)
    for g in range(NY):
        wt = wx[g].astype(F32)
        wt = jnp.concatenate([wt, jnp.zeros((BLOCK - HG, BLOCK), F32)], axis=0).T.astype(BF16)
        row = jnp.dot(pick, wt, preferred_element_type=F32)
        row = jnp.where(head_lane, row, 0.0).astype(BF16)
        wb[g] = jnp.dot(row, ones, preferred_element_type=F32)


    own_q.wait()
    for i in range(1, NY):
        q_copy(i).wait_recv()
    for g in range(NY):
        for b in range(8):
            rows = slice(b * 128, (b + 1) * 128)
            wq = (qx[g, 8 * b : 8 * b + 8].reshape(128, DH).astype(F32) * wb[g, rows, :]).astype(BF16)
            qt[:, g * RG + b * 128 : g * RG + (b + 1) * 128] = wq.T
    count = count_c.finish() * float(BLOCK * BLOCK) - float(
        4 * chips * (BLOCK * BLOCK - BLOCK * (BLOCK + 1) // 2)
    )
    scale = (LOSS_SCALE * KEYS * SCORE_SCALE) / count

    def forward(k, part_of):
        at = wrap(y - near4(k), NY)
        cols = pl.ds(pl.multiple_of(at * 512 + part_of * 256, 256), 256)
        some = pl.ds(part_of * (SLOTS // 2), SLOTS // 2)
        kv = kx[at, some].reshape(256, DH)
        keys_t = jnp.concatenate([kv[:128].T, kv[128:].T], axis=1)
        for tb in range(4):
            rows = slice(tb * 256, (tb + 1) * 256)
            acc = None
            for g in range(NY):
                qv = qx[g, 16 * tb : 16 * tb + 16].reshape(256, DH)
                d = jnp.dot(qv, keys_t, preferred_element_type=F32)
                dots[g * RG + tb * 256 : g * RG + (tb + 1) * 256, cols] = d.astype(BF16)
                wv = wb[g, rows, :]
                term = jnp.maximum(d, 0.0) * jnp.concatenate([wv, wv], axis=1)
                acc = term if acc is None else acc + term
            sc[tb * 16 : (tb + 1) * 16, cols] = (
                jnp.sum(acc.reshape(16, 16, 256), axis=1) * SCORE_SCALE
            )

    def quarter(k):
        @pl.when(k > 0)
        def _():
            k_copy(near4(k)).wait_recv()

        loop(0, 2, lambda part_of: forward(k, part_of))

    loop(0, NY, quarter)

    row = lax.broadcasted_iota(jnp.int32, (ROWS, BLOCK), 0) + half
    col = lax.broadcasted_iota(jnp.int32, (ROWS, BLOCK), 1)
    group = col // QUARTER
    chosen_on = []
    for m in range(4):
        on = jnp.zeros((ROWS, BLOCK), jnp.int32)
        for u in range(4):
            one = jnp.where(chosen_s[tile, 4 * m + u] >= 0, 1, 0)
            on = jnp.where(group == u, jnp.full((ROWS, BLOCK), one, jnp.int32), on)
        chosen_on.append(on)

    def live(p):
        q, m = p // 4, p % 4
        on = chosen_on[m]
        if m == 0:
            on = jnp.where((group > 0) | (q * QUARTER + col <= row), on, 0)
        return on > 0

    def part(j):
        return slice(j * BLOCK, (j + 1) * BLOCK)

    top = None
    tsum = None
    for j in range(SLOTS):
        s = jnp.where(live(j), sc[:, part(j)], -1e30)
        t = jnp.where(live(j), tgt[:, part(j)].astype(F32), 0.0)
        top = s if top is None else jnp.maximum(top, s)
        tsum = t if tsum is None else tsum + t
    row_max = jnp.max(top, axis=1, keepdims=True)
    row_t = 1.0 / jnp.sum(tsum, axis=1, keepdims=True)
    esum = None
    for j in range(SLOTS):
        e = jnp.where(live(j), jnp.exp(jnp.where(live(j), sc[:, part(j)] - row_max, 0.0)), 0.0)
        gs[:, part(j)] = e
        esum = e if esum is None else esum + e
    norm = jnp.sum(esum, axis=1, keepdims=True)
    row_n = 1.0 / norm
    lse = row_max + jnp.log(norm)
    kl = None
    for j in range(SLOTS):
        on = live(j)
        prob = jnp.where(on, tgt[:, part(j)].astype(F32) * row_t, 0.0)
        term = jnp.where(
            on, prob * (jnp.log(jnp.where(on, prob, 1.0)) - sc[:, part(j)] + lse), 0.0
        )
        kl = term if kl is None else kl + term
        gs[:, part(j)] = gs[:, part(j)] * row_n - prob
    kl_row = jnp.sum(kl, axis=0, keepdims=True)
    loss_y.start(jnp.broadcast_to(jnp.sum(kl_row, axis=1, keepdims=True), (1, 128)))

    def d_copy(i):
        peer = lax.rem(y + i, NY)
        return remote(dks.at[peer], yrecv.at[y], ds_.at[i], dr.at[i], {"y": peer})

    def key_grad(k, part_of):
        at = lax.rem(y + near4(NY - 1 - k), NY)
        cols = pl.ds(pl.multiple_of(at * 512 + part_of * 256, 256), 256)
        got = None
        for tb in range(4):
            grad = jnp.concatenate(
                [
                    jnp.broadcast_to(gs[tb * 16 + u : tb * 16 + u + 1, cols], (HG, 256)).astype(BF16)
                    for u in range(16)
                ],
                axis=0,
            )
            for g in range(NY):
                rows = slice(g * RG + tb * 256, g * RG + (tb + 1) * 256)
                d = dots[rows, cols]
                d = jnp.where(d > 0, grad, jnp.zeros_like(grad))
                dots[rows, cols] = d
                term = jnp.dot(qt[:, rows], d, preferred_element_type=F32)
                got = term if got is None else got + term
        for u in range(2):
            block = (got[:, u * 128 : (u + 1) * 128].T * scale).astype(BF16)
            dks[at, pl.ds(part_of * 8 + u * 4, 4)] = block.reshape(4, QUARTER, DH)

    def key_quarter(k):
        loop(0, 2, lambda part_of: key_grad(k, part_of))

        @pl.when(k < NY - 1)
        def _():
            d_copy(near4(NY - 1 - k)).start()

    loop(0, NY, key_quarter)
    loss_z.start(loss_y.finish())

    def qg_copy(i):
        peer = lax.rem(y + i, NY)
        return remote(qg.at[peer], oq.at[y], gs_.at[i], gr.at[i], {"y": peer})

    def wg_copy(i):
        peer = lax.rem(y + i, NY)
        return remote(wg.at[peer], wgr.at[y], vs.at[i], vr.at[i], {"y": peer})

    def query_grad(i):
        g = lax.rem(y + i, NY)
        rows = pl.ds(pl.multiple_of(g * RG, RG), RG)
        a = jnp.dot(dots[rows, :], kx[...].reshape(KEYS, DH), preferred_element_type=F32) * scale
        qg[g] = (a * wb[g]).astype(BF16).reshape(ROWS, HG, DH)
        s = jnp.sum(a.reshape(ROWS, HG, DH) * qx[g].astype(F32), axis=2).T
        nil = jnp.zeros((HG, ROWS), F32)
        wg[g] = jnp.where(
            half == 0, jnp.concatenate([s, nil], axis=1), jnp.concatenate([nil, s], axis=1)
        )

    for i in (2, 1, 3, 0):
        query_grad(i)
    loss_x.start(loss_z.finish())
    loop(1, nz, lambda dz: z_copy(dz).wait_send())
    loop(0, nz, lambda dz: c_copy(dz).wait_send())
    loop(nz, chips, lambda i: x_copy(i // nz, lax.rem(i, nz)).wait_send())
    for i in range(1, NY):
        q_copy(i).wait_send()
        w_copy(i).wait_send()
        k_copy(i).wait_send()
    for r in rows_of[:3]:
        r.drain()

    yrecv[y] = dks[y]
    table[2 * SLOTS] = jnp.zeros((QUARTER, DH), F32)
    for i in range(1, NY):
        d_copy(i).wait_recv()
    for i in (2, 1, 3):
        wg_copy(i).start()
        qg_copy(i).start()
    for t in range(2):
        def pair(j):
            table[t * SLOTS + j] = yrecv[2 * t, j].astype(F32) + yrecv[2 * t + 1, j].astype(F32)

        loop(0, SLOTS, pair)

    def dense(core, cx, dz, l):
        pos = slot(0, cx, lax.rem(z + dz, nz)) * 4 + core * 2 + l
        return table[inv[0, pos]] + table[inv[1, pos]]

    def e_copy(dz):
        return remote(dsend.at[dz], drecv.at[dz], es.at[dz], er.at[dz], other)

    def u_copy(dx, dz):
        to = lax.rem(x + dx, nx)
        i = dx * nz + dz
        return remote(pay.at[dz, to], xrecv.at[dx, dz], us.at[i], ur.at[i], {"x": to})

    def h_copy(dz):
        return remote(
            zsend.at[dz], zrecv.at[dz], hs.at[dz], hr.at[dz], {"z": lax.rem(z + dz, nz)}
        )

    def to_core(k):
        dz = near(nz - 1 - k)
        for cx in range(nx):
            for l in range(2):
                dsend[dz, cx, l] = dense(1 - c, cx, dz, l).astype(BF16)
        e_copy(dz).start()

    loop(0, nz, to_core)
    own_o = pltpu.make_async_copy(qg.at[y], oq.at[y], osem)
    own_o.start()
    wgr[y] = wg[y]
    loss_c.start(loss_x.finish())

    def to_x(k):
        dz = near(nz - 1 - k)
        e_copy(dz).wait_recv()
        for cx in range(nx):
            for l in range(2):
                v = dense(c, cx, dz, l) + drecv[dz, cx, l].astype(F32)
                pay[dz, cx, l] = v.astype(BF16)
        for dx in (2, 1, 3):
            u_copy(dx, dz).start()

    loop(0, nz, to_x)
    loss = loss_c.finish() * float(KEYS) / count
    ol_v[...] = jnp.broadcast_to(loss, (8, 128))

    def x_total(dz):
        total = pay[dz, x].astype(F32)
        for dx in (1, 3, 2):
            u_copy(dx, dz).wait_recv()
            total = total + xrecv[dx, dz].astype(F32)
        return total

    def to_z(k):
        dz = near(nz - 1 - k)
        zsend[dz] = x_total(dz).astype(BF16)
        h_copy(dz).start()

    loop(0, nz - 1, to_z)
    fin[...] = x_total(0)
    def add_z(k):
        dz = near(k)
        h_copy(dz).wait_recv()
        fin[...] += zrecv[dz].astype(F32)

    loop(1, nz, add_z)

    def f_copy(i):
        return remote(
            fin_b, ok.at[:, mine, :], fs.at[i], fr.at[i], {"y": lax.rem(y + i, NY)}
        )

    fin_b[...] = fin[...].astype(BF16)
    for i in (2, 1, 3):
        f_copy(i).start()

    for i in range(1, NY):
        wg_copy(i).wait_recv()
    ow_v[:, 0:128] = wgr[0] + wgr[1]
    ow_v[:, 128:256] = wgr[2] + wgr[3]
    results = [
        pltpu.make_async_copy(src, dst, rsem.at[i])
        for i, (src, dst) in enumerate(((fin_b, ok.at[:, mine, :]), (ol_v, ol), (ow_v, ow)))
    ]
    for copy in results:
        copy.start()
    own_o.wait()
    loop(nz, chips, lambda i: u_copy(i // nz, lax.rem(i, nz)).wait_send())
    loop(0, nz, lambda dz: e_copy(dz).wait_send())
    loop(1, nz, lambda dz: h_copy(dz).wait_send())
    for r in rows_of[3:]:
        r.drain()
    for i in range(1, NY):
        d_copy(i).wait_send()
        wg_copy(i).wait_send()
        qg_copy(i).wait()
    for copy in results:
        copy.wait()
    for i in range(1, NY):
        f_copy(i).wait()


def finish_kernel(q_in, w_in, k_in, l_in, q_out, w_out, k_out, l_out):
    q_out[...] = q_in[...]
    w_out[...] = w_in[...]
    k_out[...] = k_in[...].astype(F32)
    l_out[0, 0] = l_in[0, 0]


VM = pl.BlockSpec(memory_space=pltpu.VMEM)
SM = pl.BlockSpec(memory_space=pltpu.SMEM)
ANY = pl.BlockSpec(memory_space=pl.ANY)


def shape(*dims_dtype):
    return jax.ShapeDtypeStruct(dims_dtype[:-1], dims_dtype[-1])


def local(nx, nz, queries, head_weights, keys, targets, chosen, tile_block):
    chips = nx * nz
    rows = NY * ROWS
    q4 = queries.reshape(NY, ROWS, HG, DH)
    v = pltpu.VMEM
    scratch = [
        v((HG, rows), BF16), v((2, BLOCK, DH), BF16),
        v((HG, rows), F32), v((8, 128), F32), v((2, QUARTER, DH), BF16), DMA((2,)), DMA((3,)),
        v((2 * chips, 2, QUARTER, DH), BF16),
        v((2, SLOTS, QUARTER, DH), BF16),
        v((NY, ROWS, HG, DH), BF16),
        v((NY, HG, BLOCK), BF16),
        v((NY, SLOTS, QUARTER, DH), BF16),
        v((NY, RG, DH), F32),
        v((DH, NY * RG), BF16),
        v((NY * RG, KEYS), BF16),
        v((ROWS, KEYS), F32),
        v((ROWS, KEYS), F32),
        v((ROWS, KEYS), BF16),
        v((ROWS, KEYS), BF16),
        v((NY, ROWS, HG, DH), BF16),
        v((NY, HG, BLOCK), F32),
        v((NY, HG, BLOCK), F32),
        pltpu.SMEM((2, 4 * chips), jnp.int32),
        v((NY, SLOTS, QUARTER, DH), BF16),
        v((NY, SLOTS, QUARTER, DH), BF16),
        v((2 * SLOTS + 1, QUARTER, DH), F32),
        v((nz, nx, 2, QUARTER, DH), BF16),
        v((nz, nx, 2, QUARTER, DH), BF16),
        v((nz, nx, 2, QUARTER, DH), BF16),
        v((nx, nz, 2, QUARTER, DH), BF16),
        v((nz, 2, QUARTER, DH), BF16),
        v((nz, 2, QUARTER, DH), BF16),
        v((2, QUARTER, DH), F32),
        DMA, DMA, DMA,
    ]
    for n in (NY, NY, nz, chips, nz, NY, NY, NY, NY, nz, chips, nz, NY):
        scratch += [DMA((n,)), DMA((n,))]
    for n in (nz, nx, 2, NY, nz, nx, 2):
        scratch += row_sum_scratch(n)
    oq, ow, ok, ol = pl.pallas_call(
        functools.partial(kernel, nx, nz),
        out_shape=[
            shape(NY, ROWS, HG, DH, BF16),
            shape(HG, rows, F32),
            shape(2, BLOCK, DH, BF16),
            shape(8, 128, F32),
        ],
        in_specs=[ANY, ANY, ANY, ANY, SM, SM],
        out_specs=[ANY] * 4,
        scratch_shapes=scratch,
        compiler_params=pltpu.CompilerParams(
            collective_id=0, has_side_effects=True, vmem_limit_bytes=60 * 1024 * 1024
        ),
        name="step",
    )(q4, head_weights.T, keys.reshape(2, BLOCK, DH), targets.reshape(NY, ROWS, KEYS), chosen, tile_block)
    oq, ow, ok, ol = pl.pallas_call(
        finish_kernel,
        out_shape=[
            shape(NY, ROWS, HG, DH, BF16),
            shape(HG, rows, F32),
            shape(2, BLOCK, DH, F32),
            shape(1, 1, F32),
        ],
        in_specs=[VM, VM, VM, VM],
        out_specs=[VM, VM, VM, SM],
        name="finish",
    )(oq, ow, ok, ol)
    return oq.reshape(rows, HG, DH), ow.T, ok.reshape(rows, DH), ol[0, 0]


def solution(mesh):
    nx, nz = 4, mesh.shape["seq"] // 8
    torus = Mesh(mesh.devices.reshape(nx, nz, 2, mesh.shape["head"]), ("x", "z", "c", "y"))
    in_specs = (P(SEQ, "y", None), P(SEQ, "y"), P(SEQ, None), P(SEQ, None), P(SEQ, None), P())
    out_specs = (P(SEQ, "y", None), P(SEQ, "y"), P(SEQ, None), P())
    return jax.shard_map(
        functools.partial(local, nx, nz),
        mesh=torus, in_specs=in_specs, out_specs=out_specs, check_vma=False,
    )
```
